128 devices in a mesh: dp: 8 (over z_lo, x), expert: 16 (over y, z_hi, core).
Axes of the slice: x: 4, y: 4, z: 4 (z_hi: 2, z_lo: 2; z = z_hi * 2 + z_lo), core: 2. Of those that a mesh axis runs over, the one named last changes fastest.
Arguments:
- hidden: bfloat16 [16, 9216, 1408], P('expert', 'dp')
- upstream: bfloat16 [16, 9216, 2048], P('expert', 'dp')
- token_counts: int32 [16, 8], P('expert', 'dp'), may hold values from 1 to 1152, as said below
- master: float32 [16, 1408, 2048], P('expert', 'dp'), may hold values from -0.15625 to 0.15625
- first_moment: float32 [16, 1408, 2048], P('expert', 'dp'), may hold values from -6 to 6
- second_moment: float32 [16, 1408, 2048], P('expert', 'dp'), may hold values from 0.25 to 4
- router_input: bfloat16 [16384, 2048], P(('dp', 'expert')), may hold values from -6 to 6
- router_cot: bfloat16 [64, 16384], P(None, ('dp', 'expert'))
- router_master: float32 [64, 2048], replicated, may hold values from -0.125 to 0.125
- router_first: float32 [64, 2048], replicated, may hold values from -6 to 6
- router_second: float32 [64, 2048], replicated, may hold values from 0.25 to 4
- partner: int32 [16], replicated, may hold values from 0 to 15, as said below
Outputs:
- new_weight: bfloat16 [16, 1408, 2048], P('expert')
- new_master: float32 [16, 1408, 2048], P('expert', 'dp')
- new_first: float32 [16, 1408, 2048], P('expert', 'dp')
- new_second: float32 [16, 1408, 2048], P('expert', 'dp')
- router_master_new: float32 [64, 2048], replicated
- router_first_new: float32 [64, 2048], replicated
- router_second_new: float32 [64, 2048], replicated
The draws below stay inside these ranges and needn't reach their ends.
Inputs may be any that keep to these rules, and one draw needn't show every extreme that they name: partner[partner[p]] = p for every position p; a position with partner[p] = p keeps its expert. The first token_counts[e, d] of replica d's 1152 slots for position e are live, the rest are padding.
All inputs are finite; a program needn't handle non-finite values.
Results may differ from the reference program's by a relative error of at most 0.001.
Values may be sent and summed in bfloat16 or wider, within the bound.
A program may use at most 128 MiB of HBM per device.

```python
import math
import jax
import jax.numpy as jnp
from jax import lax

D = 2048
F = 1408
EXP_ALL = 64
ROWS = 1152
EXPERTS = 16
TOKENS = 16384
N_DP = 8


def draw_hidden(key, part):
    key_base = jax.random.fold_in(key, 11)
    key_column = jax.random.fold_in(key, 12)
    key_row = jax.random.fold_in(key, 13)
    shape_all = (EXPERTS, N_DP * ROWS, F)
    base_values = jax.random.normal(key_base, shape_all, jnp.float32)
    column_rise = jnp.power(3.0, jnp.arange(F, dtype=jnp.float32) / max(F - 1, 1))
    column_scale = jnp.exp(jax.random.uniform(key_column, (F,), jnp.float32, 0.0, math.log(10.0))) * column_rise
    row_scale = jnp.exp(jax.random.uniform(key_row, (EXPERTS, N_DP * ROWS, 1), jnp.float32, 0.0, math.log(4.0)))
    return (0.25 * base_values * row_scale * column_scale).astype(jnp.bfloat16)


def draw_upstream(key, part):
    key_base = jax.random.fold_in(key, 21)
    key_row = jax.random.fold_in(key, 22)
    shape_all = (EXPERTS, N_DP * ROWS, D)
    base_values = jax.random.normal(key_base, shape_all, jnp.float32)
    row_scale = jnp.exp(jax.random.uniform(key_row, (EXPERTS, N_DP * ROWS, 1), jnp.float32, 0.0, math.log(10.0)))
    expert_scale = jnp.power(3.0, jnp.arange(EXPERTS, dtype=jnp.float32) / max(EXPERTS - 1, 1))
    return (0.3 * base_values * row_scale * expert_scale[:, None, None]).astype(jnp.bfloat16)


def draw_router_cot(key, part):
    key_base = jax.random.fold_in(key, 31)
    key_column = jax.random.fold_in(key, 32)
    shape_all = (EXP_ALL, TOKENS)
    base_values = jax.random.normal(key_base, shape_all, jnp.float32)
    token_rise = jnp.power(3.0, jnp.arange(TOKENS, dtype=jnp.float32) / max(TOKENS - 1, 1))
    token_scale = jnp.exp(jax.random.uniform(key_column, (TOKENS,), jnp.float32, 0.0, math.log(10.0))) * token_rise
    return (0.3 * base_values * token_scale).astype(jnp.bfloat16)


def draw_token_counts(key, part):
    key_hot = jax.random.fold_in(key, 41)
    key_light = jax.random.fold_in(key, 42)
    hot_rank = jax.random.permutation(key_hot, EXPERTS)
    is_hot = hot_rank < max(EXPERTS // 4, 1)
    light = jax.random.randint(key_light, (EXPERTS, N_DP), 1, ROWS // 2 + 1)
    return jnp.where(is_hot[:, None], ROWS, light).astype(jnp.int32)


def draw_partner(key, part):
    key_order = jax.random.fold_in(key, 51)
    key_pairs = jax.random.fold_in(key, 52)
    order = jax.random.permutation(key_order, EXPERTS).astype(jnp.int32)
    pair_count = jax.random.randint(key_pairs, (), EXPERTS // 4, EXPERTS // 2 + 1)
    places = jnp.arange(EXPERTS, dtype=jnp.int32)
    mate_place = jnp.where(places < 2 * pair_count, jnp.bitwise_xor(places, 1), places)
    return jnp.zeros((EXPERTS,), jnp.int32).at[order].set(jnp.take(order, mate_place)).astype(jnp.int32)


def block_scale(own_key, shape, shards, low, top_value):
    gain = 1.0
    for axis_at, shards_of in shards:
        draws = jax.random.uniform(jax.random.fold_in(jax.random.fold_in(own_key, 6), axis_at), (shards_of,), jnp.float32, low / len(shards), top_value / len(shards))
        gain = gain * jnp.repeat(jnp.exp(draws), shape[axis_at] // shards_of).reshape((-1,) + (1,) * (len(shape) - 1 - axis_at))
    return gain


def scatter_about(rng, shape, scale, limit, split=(), kind=jnp.bfloat16):
    result = jax.random.normal(rng, shape, jnp.float32) * scale
    if len(split) > 0:
        result = block_scale(rng, shape, split, -0.22, 0.18) * result
    return jnp.clip(result, min=-limit, max=limit).astype(kind)


def setup_inputs(seed: int = 0) -> dict:
    splits = jax.random.split(jax.random.key(seed), 13)
    return {
        "hidden": draw_hidden(jax.random.fold_in(splits[12], 71), 0),
        "upstream": draw_upstream(jax.random.fold_in(splits[12], 71), 0),
        "token_counts": draw_token_counts(jax.random.fold_in(splits[12], 71), 0),
        "master": scatter_about(splits[3], (EXPERTS, F, D), F ** -0.5, 0.15625, ((0, 16), (1, 8)), jnp.float32),
        "first_moment": scatter_about(splits[4], (EXPERTS, F, D), 1.0, 6.0, ((0, 16), (1, 8)), jnp.float32),
        "second_moment": jnp.clip(jnp.exp(math.log(4.0) - 2.7725887 * jax.random.uniform(splits[5], (EXPERTS, F, D), jnp.float32) ** block_scale(splits[5], (EXPERTS, F, D), ((0, 16), (1, 8)), -0.2, 0.2)), 0.25, 4.0),
        "router_input": scatter_about(splits[6], (TOKENS, D), 1.0, 6.0, ((0, 128),)),
        "router_cot": draw_router_cot(jax.random.fold_in(splits[12], 71), 0),
        "router_master": scatter_about(splits[8], (EXP_ALL, D), D ** -0.5, 0.125, (), jnp.float32),
        "router_first": scatter_about(splits[9], (EXP_ALL, D), 1.0, 6.0, (), jnp.float32),
        "router_second": jnp.clip(jnp.exp(jax.random.uniform(splits[10], (EXP_ALL, D), jnp.float32, math.log(0.25), math.log(4.0))), 0.25, 4.0),
        "partner": draw_partner(jax.random.fold_in(splits[12], 71), 0),
    }


beta_first = 0.9
beta_second = 0.95
learn_rate = 0.001
decay_weight = 0.1
adam_eps = 1e-08
norm_eps = 1e-06
correct_first = 1.0 - 0.9 ** 10
correct_second = 1.0 - 0.95 ** 10

def adam_update(gradient, moment_one, moment_two, weights):
    first_new = beta_first * moment_one + (1.0 - beta_first) * gradient
    second_new = beta_second * moment_two + (1.0 - beta_second) * gradient * gradient
    ratio = first_new / correct_first / (jnp.sqrt(second_new / correct_second) + adam_eps)
    weights_new = weights - learn_rate * (ratio + decay_weight * weights)
    return (weights_new, first_new, second_new)

def reference(hidden, upstream, token_counts, master, first_moment, second_moment, router_input, router_cot, router_master, router_first, router_second, partner):
    row_index = jnp.arange(N_DP * ROWS, dtype=jnp.int32)
    within = row_index % ROWS
    replica = row_index // ROWS

    def expert_grad(packed):
        activations, grads_out, counts = packed
        live_rows = within < jnp.take(counts, replica)
        masked = jnp.where(live_rows[:, None], activations, jnp.zeros_like(activations))
        return jnp.dot(masked.T, grads_out, preferred_element_type=jnp.float32)
    gradient = lax.map(expert_grad, (hidden, upstream, token_counts))
    router_grad = jnp.dot(router_cot, router_input, preferred_element_type=jnp.float32)
    total_square = jnp.sum(gradient * gradient) + jnp.sum(router_grad * router_grad)
    clip_limit = 2.0 * math.sqrt(float(EXPERTS * F * D + EXP_ALL * D))
    factor = jnp.minimum(1.0, clip_limit / (jnp.sqrt(total_square) + norm_eps))
    master_new, first_new, second_new = adam_update(factor * gradient, first_moment, second_moment, master)
    router_outs = adam_update(factor * router_grad, router_first, router_second, router_master)
    moved_master = jnp.take(master_new, partner, axis=0)
    moved_first = jnp.take(first_new, partner, axis=0)
    moved_second = jnp.take(second_new, partner, axis=0)
    return (moved_master.astype(jnp.bfloat16), moved_master, moved_first, moved_second, router_outs[0], router_outs[1], router_outs[2])
```

```python
import functools
import math

import jax
import jax.numpy as jnp
from jax import lax
from jax.experimental import pallas as pl
from jax.experimental.pallas import tpu as pltpu
from jax.sharding import Mesh
from jax.sharding import PartitionSpec as P

MESH = pl.DeviceIdType.MESH
DP = ("zl", "x")
ALL = ("zl", "x", "e")
F32 = jnp.float32
I16 = jnp.int16

beta_first = 0.9
beta_second = 0.95
learn_rate = 0.001
decay_weight = 0.1
adam_eps = 1e-08
norm_eps = 1e-06
correct_first = 1.0 - 0.9**10
correct_second = 1.0 - 0.95**10

GROUPS = 16
LANES = 128
TOP = 15.0
SMALL = 2.0**-100


def code_of(peak):
    return jnp.ceil(16.0 * jnp.log2(jnp.maximum(peak, SMALL)))


def to_codes(values, code):
    scaled = jnp.round(values * jnp.exp2(TOP - code * (1.0 / 16.0)))
    return jnp.clip(scaled, -32767.0, 32767.0).astype(I16)


def scale_of(code):
    return jnp.exp2(code * (1.0 / 16.0) - TOP)


def encode_rows(values, dst, rows):
    width = values.shape[1]
    code = code_of(jnp.max(jnp.abs(values), axis=1, keepdims=True))
    dst[rows, :width] = to_codes(values, code)
    dst[rows, width:] = jnp.broadcast_to(code, (values.shape[0], LANES)).astype(I16)


def decode_rows(src, rows, width):
    code = src[rows, width : width + LANES].astype(F32)[:, :1]
    return src[rows, :width].astype(F32) * scale_of(code)


def cut(rows):
    tiles = rows // 16
    first = (tiles + 1) // 2 * 16
    return ((0, first), (first, rows - first))


def send(src, dst, send_sem, recv_sem, device):
    copy = pltpu.make_async_remote_copy(
        src_ref=src, dst_ref=dst, send_sem=send_sem, recv_sem=recv_sem, device_id=device, device_id_type=MESH
    )
    copy.start()
    return copy


def reduce_kernel(
    hid,
    up,
    counts,
    cot,
    rin,
    grad,
    rgrad,
    total,
    hid_t,
    part,
    held,
    out_buf,
    in_buf,
    rp,
    rx,
    r1,
    rz,
    r2,
    ry,
    r3,
    rc,
    sums,
    ssem,
    rsem,
    r_ssem,
    r_rsem,
    n_ssem,
    n_rsem,
):
    zl, x, e = (lax.axis_index(a) for a in ALL)
    y, zh, core = e // 4, (e // 2) % 2, e % 2
    z = zh * 2 + zl
    depth, units = hid.shape
    wide = up.shape[1]
    rows = units // 8

    def at_x(j):
        return {"x": (x + j) % 4}

    def at_z(j):
        there = (z + j) % 4
        return {"zl": there % 2, "e": y * 4 + (there // 2) * 2 + core}

    def at_y(j):
        return {"e": ((y + j) % 4) * 4 + zh * 2 + core}

    def at_core(j):
        return {"e": e + 1 - 2 * core}

    def at_pair():
        return {"zl": 1 - zl}

    axes = ((at_x, 4, x), (at_z, 4, z), (at_y, 4, y), (at_core, 2, core))

    barrier = pltpu.get_barrier_semaphore()
    for at, size, _ in axes:
        for j in range(1, size):
            pl.semaphore_signal(barrier, inc=1, device_id=at(j), device_id_type=MESH)

    rp[...] = jnp.dot(cot[...], rin[...], preferred_element_type=F32)
    pl.semaphore_wait(barrier, 10)

    r_rows, r_cols = rp.shape[0] // 4, wide // 4
    stage0 = [
        send(
            rp.at[pl.ds(((x + j) % 4) * r_rows, r_rows)],
            rx.at[j - 1],
            r_ssem.at[0, j],
            r_rsem.at[0, j],
            at_x(j),
        )
        for j in range(1, 4)
    ]

    live = counts[0, 0]

    @pl.loop(0, units // LANES)
    def _(t):
        cols = pl.ds(pl.multiple_of(t * LANES, LANES), LANES)
        keep = lax.broadcasted_iota(jnp.int32, (depth, LANES), 0) < live
        tile = jnp.where(keep, hid[:, cols].astype(F32), 0.0).astype(jnp.bfloat16)
        hid_t[cols, :] = tile.T

    def multiply(block, dst):
        at = pl.multiple_of(block * rows, 16)

        @pl.loop(0, wide // 512)
        def _(n):
            cols = pl.ds(pl.multiple_of(n * 512, 512), 512)
            dst[:, cols] = jnp.dot(hid_t[pl.ds(at, rows), :], up[:, cols], preferred_element_type=F32)

    def encode(src, slot, run, *incoming):
        start, size = run

        @pl.loop(0, size // 16)
        def _(i):
            r = pl.ds(pl.multiple_of(start + i * 16, 16), 16)
            values = src[r, :]
            for b in incoming:
                values = values + decode_rows(in_buf.at[b], r, wide)
            encode_rows(values, out_buf.at[slot], r)

    def ship(slot, run, c, device):
        r = pl.ds(run[0], run[1])
        return send(out_buf.at[slot, r], in_buf.at[slot, r], ssem.at[slot, c], rsem.at[slot, c], device)

    runs = cut(rows)
    far, right, left = (x + 2) % 4, (x + 1) % 4, (x + 3) % 4
    copies = {}
    for slot, block, step in ((0, far, 3), (1, 4 + far, 1), (2, right, 1), (3, 4 + left, 3)):
        multiply(block, part)
        for c, run in enumerate(runs):
            encode(part, slot, run)
            copies[slot, c] = ship(slot, run, c, at_x(step))
    multiply(left, held.at[0])
    multiply(4 + right, held.at[1])

    for copy in stage0:
        copy.wait_recv()
    r1[...] = rp[pl.ds(x * r_rows, r_rows), :] + rx[0] + rx[1] + rx[2]
    stage1 = [
        send(
            r1.at[:, pl.ds(pl.multiple_of(((z + j) % 4) * r_cols, LANES), r_cols)],
            rz.at[j - 1],
            r_ssem.at[1, j],
            r_rsem.at[1, j],
            at_z(j),
        )
        for j in range(1, 4)
    ]

    for c, run in enumerate(runs):
        for slot, step in ((4, 3), (5, 1)):
            copies[slot - 4, c].wait_recv()
            encode(held.at[slot - 4], slot, run, slot - 4)
            copies[slot, c] = ship(slot, run, c, at_x(step))

    multiply(x, held.at[2])
    multiply(4 + x, held.at[3])

    for copy in stage1:
        copy.wait_recv()
    r2[...] = r1[:, pl.ds(pl.multiple_of(z * r_cols, LANES), r_cols)] + rz[0] + rz[1] + rz[2]
    stage2 = [
        send(
            r2.at[:, pl.ds(pl.multiple_of(((y + j) % 4) * LANES, LANES), LANES)],
            ry.at[j - 1],
            r_ssem.at[2, j],
            r_rsem.at[2, j],
            at_y(j),
        )
        for j in range(1, 4)
    ]
    for copy in stage2:
        copy.wait_recv()
    r3[...] = r2[:, pl.ds(pl.multiple_of(y * LANES, LANES), LANES)] + ry[0] + ry[1] + ry[2]
    other = pl.multiple_of((1 - core) * 8, 8)
    stage3 = send(r3.at[pl.ds(other, 8)], rc, r_ssem.at[3, 1], r_rsem.at[3, 1], at_core(1))

    for c, run in enumerate(runs):
        copies[2, c].wait_recv()
        copies[4, c].wait_recv()
        copies[3, c].wait_recv()
        copies[5, c].wait_recv()

        @pl.loop(0, run[1] // 16)
        def _(i, run=run):
            r = pl.ds(pl.multiple_of(run[0] + i * 16, 16), 16)
            held[2, r, :] += decode_rows(in_buf.at[2], r, wide) + decode_rows(in_buf.at[4], r, wide)
            held[3, r, :] += decode_rows(in_buf.at[3], r, wide) + decode_rows(in_buf.at[5], r, wide)

        encode(held.at[3 - zl], 6, run)
        copies[6, c] = ship(6, run, c, at_pair())

    stage3.wait_recv()
    piece = r3[pl.ds(pl.multiple_of(core * 8, 8), 8), :] + rc[...]
    my_rows, my_cols = x * r_rows + core * 8, z * r_cols + y * LANES
    rgrad[pl.ds(pl.multiple_of(my_rows, 8), 8), pl.ds(pl.multiple_of(my_cols, LANES), LANES)] = piece

    def spread(row, height, col, width, stage, at, size):
        part_of = rgrad.at[
            pl.ds(pl.multiple_of(row, 8), height), pl.ds(pl.multiple_of(col, LANES), width)
        ]
        return [
            send(part_of, part_of, r_ssem.at[stage, j], r_rsem.at[stage, j], at(j)) for j in range(1, size)
        ]

    back = [spread(my_rows, 8, my_cols, LANES, 4, at_core, 2)]

    squares = piece * piece
    for c, run in enumerate(runs):
        copies[6, c].wait_recv()

        def add(i, acc, run=run):
            r = pl.ds(pl.multiple_of(run[0] + i * 16, 16), 16)
            values = held[2 + zl, r, :] + decode_rows(in_buf.at[6], r, wide)
            grad[r, :] = values
            values = values * values
            for a in range(2):
                for b in range(wide // LANES):
                    acc = acc + values[a * 8 : a * 8 + 8, b * LANES : (b + 1) * LANES]
            return acc

        squares = lax.fori_loop(0, run[1] // 16, add, squares)

    norm_copies = []
    spreads = (
        (x * r_rows, 2 * 8, my_cols, LANES, 5, at_y, 4),
        (x * r_rows, r_rows, z * r_cols, r_cols, 6, at_z, 4),
        (x * r_rows, r_rows, 0, wide, 7, at_x, 4),
    )
    for stage, (at, size, here) in enumerate(axes):
        sums[stage, here] = squares
        mine = sums.at[stage, here]
        group = [
            send(mine, mine, n_ssem.at[stage, j], n_rsem.at[stage, j], at(j)) for j in range(1, size)
        ]
        norm_copies += group
        if stage < 3:
            for copy in back[-1]:
                copy.wait_recv()
            back.append(spread(*spreads[stage]))
        for copy in group:
            copy.wait_recv()
        squares = sums[stage, 0]
        for k in range(1, size):
            squares = squares + sums[stage, k]
    total[...] = jnp.broadcast_to(jnp.sum(squares), total.shape)
    for copy in back[-1]:
        copy.wait_recv()
    for copy in list(copies.values()) + stage0 + stage1 + stage2 + [stage3] + norm_copies + sum(back, []):
        copy.wait_send()


def move_kernel(
    limit,
    grad,
    total,
    master,
    first,
    second,
    partner,
    weight,
    rest,
    high_out,
    high_in,
    high_to,
    rest_out,
    rest_in,
    rest_to,
    ssem,
    rsem,
    a_ssem,
    a_rsem,
):
    zl, x, e = (lax.axis_index(a) for a in ALL)
    rows, wide = grad.shape
    half = wide // 2
    tall = rows + 16

    def peer(j):
        return {"e": (e + j) % GROUPS}

    def at_x(j):
        return {"x": (x + j) % 4}

    pair = {"zl": 1 - zl}

    barrier = pltpu.get_barrier_semaphore()

    def greet(j, carry):
        pl.semaphore_signal(barrier, inc=1, device_id=peer(j), device_id_type=MESH)
        return carry

    lax.fori_loop(1, GROUPS, greet, 0)
    for device in (at_x(1), at_x(3), pair):
        pl.semaphore_signal(barrier, inc=1, device_id=device, device_id_type=MESH)

    factor = jnp.minimum(1.0, limit / (jnp.sqrt(total[0:1, 0:1]) + norm_eps))

    @pl.loop(0, GROUPS)
    def _(g):
        cols = pl.ds(pl.multiple_of(g * LANES, LANES), LANES)
        gradient = factor * grad[:, cols]
        first_new = beta_first * first[:, cols] + (1.0 - beta_first) * gradient
        second_new = beta_second * second[:, cols] + (1.0 - beta_second) * gradient * gradient
        ratio = first_new / correct_first / (jnp.sqrt(second_new / correct_second) + adam_eps)
        weights = master[:, cols]
        master_new = weights - learn_rate * (ratio + decay_weight * weights)
        high = master_new.astype(jnp.bfloat16)
        high_out[g] = high
        for k, values in enumerate((master_new - high.astype(F32), first_new, second_new)):
            code = code_of(jnp.max(jnp.abs(values), axis=0, keepdims=True))
            rest_out[g, k * tall : k * tall + rows, :] = to_codes(values, code)
            rest_out[g, k * tall + rows : (k + 1) * tall, :] = jnp.broadcast_to(code, (16, LANES)).astype(I16)

    pl.semaphore_wait(barrier, GROUPS + 2)

    def out_copy(src, dst, k, j):
        return pltpu.make_async_remote_copy(
            src_ref=src.at[(e + j) % GROUPS],
            dst_ref=dst.at[j],
            send_sem=ssem.at[k, j],
            recv_sem=rsem.at[k, j],
            device_id=peer(j),
            device_id_type=MESH,
        )

    my_rows = (zl * 4 + x) * rows

    def weight_part(block, col, width):
        return weight.at[
            pl.ds(pl.multiple_of(block * rows, 16), rows), pl.ds(pl.multiple_of(col, LANES), width)
        ]

    def back_copy(k, j):
        if k == 2:
            src, dst = high_to.at[(e + j) % GROUPS], weight_part(zl * 4 + x, e * LANES, LANES)
        else:
            src, dst = rest_to.at[(e + j) % GROUPS], rest.at[:, pl.ds(pl.multiple_of(e * LANES, LANES), LANES)]
        return pltpu.make_async_remote_copy(
            src_ref=src,
            dst_ref=dst,
            send_sem=ssem.at[k, j],
            recv_sem=rsem.at[k, j],
            device_id=peer(j),
            device_id_type=MESH,
        )

    def each(act):
        def step(j, carry):
            act(j)
            return carry

        lax.fori_loop(1, GROUPS, step, 0)

    def permute(own, arrived, to):
        def step(p, carry):
            distance = (e - partner[p] + GROUPS) % GROUPS
            to[p] = arrived[distance]
            return carry

        arrived[0] = own[e]
        lax.fori_loop(0, GROUPS, step, 0)

    each(lambda j: out_copy(high_out, high_in, 0, j).start())
    each(lambda j: out_copy(high_out, high_in, 0, j).wait_recv())
    permute(high_out, high_in, high_to)
    each(lambda j: back_copy(2, j).start())
    mine = pl.ds(pl.multiple_of(e * LANES, LANES), LANES)
    weight[pl.ds(pl.multiple_of(my_rows, 16), rows), mine] = high_to[e]
    each(lambda j: out_copy(rest_out, rest_in, 1, j).start())
    each(lambda j: back_copy(2, j).wait_recv())

    def gather(n, block, col, width, device):
        part = weight_part(block, col, width)
        return send(part, part, a_ssem.at[n], a_rsem.at[n], device)

    own, twin = zl * 4 + x, (1 - zl) * 4 + x
    left, right = (x + 3) % 4, (x + 1) % 4
    g_pair = gather(0, own, 0, wide, pair)
    g_right = gather(1, own, 0, wide, at_x(1))
    g_left = gather(2, own, 0, wide, at_x(3))

    g_pair.wait_recv()
    t_right = gather(3, twin, 0, wide, at_x(1))
    t_left = gather(4, twin, 0, wide, at_x(3))
    g_right.wait_recv()
    f_right = gather(5, zl * 4 + left, 0, half, at_x(1))
    g_left.wait_recv()
    f_left = gather(6, zl * 4 + right, half, half, at_x(3))

    each(lambda j: out_copy(rest_out, rest_in, 1, j).wait_recv())
    permute(rest_out, rest_in, rest_to)
    each(lambda j: back_copy(3, j).start())
    rest[:, mine] = rest_to[e]

    t_right.wait_recv()
    h_right = gather(7, (1 - zl) * 4 + left, 0, half, at_x(1))
    t_left.wait_recv()
    h_left = gather(8, (1 - zl) * 4 + right, half, half, at_x(3))
    each(lambda j: back_copy(3, j).wait_recv())
    for copy in (f_right, f_left, h_right, h_left):
        copy.wait_recv()
    each(lambda j: out_copy(high_out, high_in, 0, j).wait_send())
    each(lambda j: out_copy(rest_out, rest_in, 1, j).wait_send())
    each(lambda j: back_copy(2, j).wait_send())
    each(lambda j: back_copy(3, j).wait_send())
    for copy in (g_pair, g_right, g_left, t_right, t_left, f_right, f_left, h_right, h_left):
        copy.wait_send()


def adam_update(gradient, moment_one, moment_two, weights):
    first_new = beta_first * moment_one + (1.0 - beta_first) * gradient
    second_new = beta_second * moment_two + (1.0 - beta_second) * gradient * gradient
    ratio = first_new / correct_first / (jnp.sqrt(second_new / correct_second) + adam_eps)
    weights_new = weights - learn_rate * (ratio + decay_weight * weights)
    return (weights_new, first_new, second_new)


def on_device(
    hidden,
    upstream,
    token_counts,
    master,
    first_moment,
    second_moment,
    router_input,
    router_cot,
    router_master,
    router_first,
    router_second,
    partner,
):
    depth, units = hidden.shape[1:]
    wide = upstream.shape[2]
    rows = units // 8
    n_router = router_cot.shape[0]
    vmem = pl.BlockSpec(memory_space=pltpu.VMEM)
    smem = pl.BlockSpec(memory_space=pltpu.SMEM)
    dma = pltpu.SemaphoreType.DMA
    coded = wide + LANES
    r_rows, r_cols = n_router // 4, wide // 4
    gradient, router_grad, total = pl.pallas_call(
        reduce_kernel,
        out_shape=(
            jax.ShapeDtypeStruct((rows, wide), F32),
            jax.ShapeDtypeStruct((n_router, wide), F32),
            jax.ShapeDtypeStruct((8, LANES), F32),
        ),
        in_specs=[vmem, vmem, smem, vmem, vmem],
        out_specs=(vmem, vmem, vmem),
        scratch_shapes=[
            pltpu.VMEM((units, depth), jnp.bfloat16),
            pltpu.VMEM((rows, wide), F32),
            pltpu.VMEM((4, rows, wide), F32),
            pltpu.VMEM((7, rows, coded), I16),
            pltpu.VMEM((7, rows, coded), I16),
            pltpu.VMEM((n_router, wide), F32),
            pltpu.VMEM((3, r_rows, wide), F32),
            pltpu.VMEM((r_rows, wide), F32),
            pltpu.VMEM((3, r_rows, r_cols), F32),
            pltpu.VMEM((r_rows, r_cols), F32),
            pltpu.VMEM((3, r_rows, LANES), F32),
            pltpu.VMEM((r_rows, LANES), F32),
            pltpu.VMEM((8, LANES), F32),
            pltpu.VMEM((4, 4, 8, LANES), F32),
            dma((7, 2)),
            dma((7, 2)),
            dma((8, 4)),
            dma((8, 4)),
            dma((4, 4)),
            dma((4, 4)),
        ],
        compiler_params=pltpu.CompilerParams(
            collective_id=0, has_side_effects=True, vmem_limit_bytes=60 * 1024 * 1024
        ),
        name="reduce",
    )(hidden[0], upstream[0], token_counts, router_cot, router_input)

    clip_limit = 2.0 * math.sqrt(float(GROUPS * units * wide + n_router * wide))
    tall = rows + 16
    weight, rest = pl.pallas_call(
        functools.partial(move_kernel, clip_limit),
        out_shape=(
            jax.ShapeDtypeStruct((units, wide), jnp.bfloat16),
            jax.ShapeDtypeStruct((3 * tall, wide), I16),
        ),
        in_specs=[vmem, vmem, vmem, vmem, vmem, smem],
        out_specs=(vmem, vmem),
        scratch_shapes=[
            *[pltpu.VMEM((GROUPS, rows, LANES), jnp.bfloat16)] * 3,
            *[pltpu.VMEM((GROUPS, 3 * tall, LANES), I16)] * 3,
            dma((4, GROUPS)),
            dma((4, GROUPS)),
            dma((9,)),
            dma((9,)),
        ],
        compiler_params=pltpu.CompilerParams(
            collective_id=1, has_side_effects=True, vmem_limit_bytes=60 * 1024 * 1024
        ),
        name="move",
    )(gradient, total, master[0], first_moment[0], second_moment[0], partner)

    factor = jnp.minimum(1.0, clip_limit / (jnp.sqrt(total[0, 0]) + norm_eps))
    router_outs = adam_update(factor * router_grad, router_first, router_second, router_master)

    def decoded(k):
        codes = rest[k * tall : k * tall + rows].astype(F32)
        return codes * scale_of(rest[k * tall + rows : k * tall + rows + 1].astype(F32))

    own = lax.axis_index("zl") * 4 + lax.axis_index("x")
    high = lax.dynamic_slice_in_dim(weight, own * rows, rows, 0)
    new_master = high.astype(F32) + decoded(0)
    return (
        weight[None],
        new_master[None],
        decoded(1)[None],
        decoded(2)[None],
        router_outs[0],
        router_outs[1],
        router_outs[2],
    )


def solution(mesh):
    split = Mesh(mesh.devices.reshape(2, 4, mesh.shape["expert"]), ALL)
    return jax.shard_map(
        on_device,
        mesh=split,
        in_specs=(
            P("e", DP, None),
            P("e", DP, None),
            P("e", DP),
            P("e", DP, None),
            P("e", DP, None),
            P("e", DP, None),
            P(ALL, None),
            P(None, ALL),
            P(),
            P(),
            P(),
            P(),
        ),
        out_specs=(
            P("e", None, None),
            P("e", DP, None),
            P("e", DP, None),
            P("e", DP, None),
            P(),
            P(),
            P(),
        ),
        check_vma=False,
    )
```

```python
import functools
import math

import jax
import jax.numpy as jnp
from jax import lax
from jax.experimental import pallas as pl
from jax.experimental.pallas import tpu as pltpu
from jax.sharding import Mesh
from jax.sharding import PartitionSpec as P

MESH = pl.DeviceIdType.MESH
DP = ("zl", "x")
ALL = ("zl", "x", "e")
F32 = jnp.float32
I16 = jnp.int16

beta_first = 0.9
beta_second = 0.95
learn_rate = 0.001
decay_weight = 0.1
adam_eps = 1e-08
norm_eps = 1e-06
correct_first = 1.0 - 0.9**10
correct_second = 1.0 - 0.95**10

GROUPS = 16
LANES = 128
TOP = 15.0
SMALL = 2.0**-100


def code_of(peak):
    return jnp.ceil(16.0 * jnp.log2(jnp.maximum(peak, SMALL)))


def to_codes(values, code):
    scaled = jnp.round(values * jnp.exp2(TOP - code * (1.0 / 16.0)))
    return jnp.clip(scaled, -32767.0, 32767.0).astype(I16)


def scale_of(code):
    return jnp.exp2(code * (1.0 / 16.0) - TOP)


def encode_rows(values, dst, rows):
    width = values.shape[1]
    code = code_of(jnp.max(jnp.abs(values), axis=1, keepdims=True))
    dst[rows, :width] = to_codes(values, code)
    dst[rows, width:] = jnp.broadcast_to(code, (values.shape[0], LANES)).astype(I16)


def decode_rows(src, rows, width):
    code = src[rows, width : width + LANES].astype(F32)[:, :1]
    return src[rows, :width].astype(F32) * scale_of(code)


def send(src, dst, send_sem, recv_sem, device):
    copy = pltpu.make_async_remote_copy(
        src_ref=src, dst_ref=dst, send_sem=send_sem, recv_sem=recv_sem, device_id=device, device_id_type=MESH
    )
    copy.start()
    return copy


def reduce_kernel(
    hid,
    up,
    counts,
    cot,
    rin,
    grad,
    rgrad,
    total,
    hid_t,
    terms,
    x_out,
    x_in,
    late_out,
    late_in,
    z_out,
    z_in,
    last_out,
    last_in,
    rp,
    r_in0,
    r1,
    r_in1,
    r2,
    r_in2,
    r3,
    r_in3,
    sums,
    x_ssem,
    x_rsem,
    z_ssem,
    z_rsem,
    r_ssem,
    r_rsem,
    n_ssem,
    n_rsem,
):
    zl, x, e = (lax.axis_index(a) for a in ALL)
    y, zh, core = e // 4, (e // 2) % 2, e % 2
    z = zh * 2 + zl
    depth, units = hid.shape
    wide = up.shape[1]
    rows = units // 8
    early = x_out.shape[1]
    late = rows - early
    late_a = late_out.shape[1]
    late_b = late - late_a

    def at_x(j):
        return {"x": (x + j) % 4}

    def at_z(j):
        there = (z + j) % 4
        return {"zl": there % 2, "e": y * 4 + (there // 2) * 2 + core}

    def at_y(j):
        return {"e": ((y + j) % 4) * 4 + zh * 2 + core}

    def at_core(j):
        return {"e": e + 1 - 2 * core}

    pair = {"zl": 1 - zl}
    axes = ((at_x, 4, x), (at_z, 4, z), (at_y, 4, y), (at_core, 2, core))

    barrier = pltpu.get_barrier_semaphore()
    for at, size, _ in axes:
        for j in range(1, size):
            pl.semaphore_signal(barrier, inc=1, device_id=at(j), device_id_type=MESH)

    live = counts[0, 0]
    keep = (lax.broadcasted_iota(jnp.int32, (depth, LANES), 0) < live).astype(F32).astype(jnp.bfloat16)

    @pl.loop(0, units // LANES)
    def _(t):
        cols = pl.ds(pl.multiple_of(t * LANES, LANES), LANES)
        hid_t[cols, :] = (hid[:, cols] * keep).T

    def multiply(block):
        at = pl.multiple_of(block * rows, 16)

        @pl.loop(0, wide // 512)
        def _(n):
            cols = pl.ds(pl.multiple_of(n * 512, 512), 512)
            terms[block, :, cols] = jnp.dot(hid_t[pl.ds(at, rows), :], up[:, cols], preferred_element_type=F32)

    def tiles(start, size, act):
        @pl.loop(0, size // 16, unroll=True)
        def _(i):
            act(
                pl.ds(pl.multiple_of(start + i * 16, 16), 16),
                pl.ds(pl.multiple_of(i * 16, 16), 16),
            )

    def x_copy(slot, device):
        return send(x_out.at[slot], x_in.at[slot], x_ssem.at[slot], x_rsem.at[slot], device)

    def late_copy(slot, size, device):
        r = pl.ds(0, size)
        return send(
            late_out.at[slot, r], late_in.at[slot, r], x_ssem.at[6 + slot], x_rsem.at[6 + slot], device
        )

    def early_part(block, slot, step, incoming=None):
        def act(r, i):
            values = terms[block, r, :]
            if incoming is not None:
                values = values + decode_rows(x_in.at[incoming], i, wide)
            encode_rows(values, x_out.at[slot], i)

        tiles(0, early, act)
        return x_copy(slot, at_x(step))

    def pair_part(n, there):
        def act(r, i):
            encode_rows(terms[(1 - zl) * 4 + there, r, :], z_out.at[n], i)

        tiles(early, late, act)
        return send(z_out.at[n], z_in.at[n], z_ssem.at[n], z_rsem.at[n], pair)

    def pair_sum(n, there):
        block = zl * 4 + there

        def act(r, i):
            terms[block, r, :] += decode_rows(z_in.at[n], i, wide)

        tiles(early, late, act)

    def late_part(there, start, size, slot, step, incoming=None):
        block = zl * 4 + there

        def act(r, i):
            values = terms[block, r, :]
            if incoming is not None:
                values = values + decode_rows(late_in.at[incoming], i, wide)
            encode_rows(values, late_out.at[slot], i)

        tiles(start, size, act)
        return late_copy(slot, size, at_x(step))

    far, right, left = (x + 2) % 4, (x + 1) % 4, (x + 3) % 4
    a_at, b_at = early, early + late_a

    multiply(far)
    pl.semaphore_wait(barrier, 10)
    e0 = early_part(far, 0, 3)
    multiply(4 + far)
    e1 = early_part(4 + far, 1, 1)
    p0 = pair_part(0, far)
    multiply(right)
    e2 = early_part(right, 2, 1)
    multiply(4 + left)
    e3 = early_part(4 + left, 3, 3)
    multiply(4 + right)
    p1 = pair_part(1, right)

    rp[...] = jnp.dot(cot[...], rin[...], preferred_element_type=F32)
    n_router = rp.shape[0]
    r_half, r_cols = n_router // 2, wide // 4
    s0 = send(
        rp.at[pl.ds(pl.multiple_of((1 - core) * r_half, 8), r_half)],
        r_in0,
        r_ssem.at[0, 1],
        r_rsem.at[0, 1],
        at_core(1),
    )
    multiply(left)
    p2 = pair_part(2, left)
    s0.wait_recv()
    r1[...] = rp[pl.ds(pl.multiple_of(core * r_half, 8), r_half), :] + r_in0[...]
    s1 = [
        send(
            r1.at[pl.ds(pl.multiple_of(((y + j) % 4) * 8, 8), 8)],
            r_in1.at[j - 1],
            r_ssem.at[1, j],
            r_rsem.at[1, j],
            at_y(j),
        )
        for j in range(1, 4)
    ]
    multiply(x)
    multiply(4 + x)
    p3 = pair_part(3, x)

    e0.wait_recv()
    e4 = early_part(left, 4, 3, 0)
    e1.wait_recv()
    e5 = early_part(4 + right, 5, 1, 1)
    p0.wait_recv()
    pair_sum(0, far)
    l0 = late_part(far, a_at, late_a, 0, 3)
    l1 = late_part(far, b_at, late_b, 1, 1)

    for copy in s1:
        copy.wait_recv()
    r2[...] = r1[pl.ds(pl.multiple_of(y * 8, 8), 8), :] + r_in1[0] + r_in1[1] + r_in1[2]
    s2 = [
        send(
            r2.at[:, pl.ds(pl.multiple_of(((z + j) % 4) * r_cols, LANES), r_cols)],
            r_in2.at[j - 1],
            r_ssem.at[2, j],
            r_rsem.at[2, j],
            at_z(j),
        )
        for j in range(1, 4)
    ]
    p1.wait_recv()
    pair_sum(1, right)
    l2 = late_part(right, a_at, late_a, 2, 1)
    p2.wait_recv()
    pair_sum(2, left)
    l3 = late_part(left, b_at, late_b, 3, 3)

    for copy in (e2, e3, e4, e5):
        copy.wait_recv()

    def fold(r, i):
        terms[x, r, :] += decode_rows(x_in.at[2], i, wide) + decode_rows(x_in.at[4], i, wide)
        terms[4 + x, r, :] += decode_rows(x_in.at[3], i, wide) + decode_rows(x_in.at[5], i, wide)
        encode_rows(terms[(1 - zl) * 4 + x, r, :], last_out, i)

    tiles(0, early, fold)
    last = send(last_out, last_in, z_ssem.at[4], z_rsem.at[4], pair)

    l0.wait_recv()
    l4 = late_part(left, a_at, late_a, 4, 3, 0)
    l1.wait_recv()
    l5 = late_part(right, b_at, late_b, 5, 1, 1)
    p3.wait_recv()
    pair_sum(3, x)

    for copy in s2:
        copy.wait_recv()
    r3[...] = r2[:, pl.ds(pl.multiple_of(z * r_cols, LANES), r_cols)] + r_in2[0] + r_in2[1] + r_in2[2]
    s3 = [
        send(
            r3.at[:, pl.ds(pl.multiple_of(((x + j) % 4) * LANES, LANES), LANES)],
            r_in3.at[j - 1],
            r_ssem.at[3, j],
            r_rsem.at[3, j],
            at_x(j),
        )
        for j in range(1, 4)
    ]

    own = zl * 4 + x

    def count(values, acc):
        values = values * values
        for a in range(2):
            for b in range(wide // LANES):
                acc = acc + values[a * 8 : a * 8 + 8, b * LANES : (b + 1) * LANES]
        return acc

    def close(start, size, acc, sources):
        def step(n, acc):
            i = pl.ds(pl.multiple_of(n * 16, 16), 16)
            r = pl.ds(pl.multiple_of(start + n * 16, 16), 16)
            values = terms[own, r, :]
            for source in sources:
                values = values + decode_rows(source, i, wide)
            grad[r, :] = values
            return count(values, acc)

        return lax.fori_loop(0, size // 16, step, acc, unroll=True)

    squares = jnp.zeros((8, LANES), F32)
    last.wait_recv()
    squares = close(0, early, squares, (last_in,))
    for copy in (l2, l4):
        copy.wait_recv()
    squares = close(a_at, late_a, squares, (late_in.at[2], late_in.at[4]))
    for copy in (l3, l5):
        copy.wait_recv()
    squares = close(b_at, late_b, squares, (late_in.at[3], late_in.at[5]))

    for copy in s3:
        copy.wait_recv()
    piece = r3[:, pl.ds(pl.multiple_of(x * LANES, LANES), LANES)] + r_in3[0] + r_in3[1] + r_in3[2]
    squares = squares + piece * piece
    my_row = core * r_half + y * 8
    z_col = z * r_cols
    x_col = z_col + x * LANES
    rgrad[pl.ds(pl.multiple_of(my_row, 8), 8), pl.ds(pl.multiple_of(x_col, LANES), LANES)] = piece

    waits = [e0, e1, e2, e3, e4, e5, l0, l1, l2, l3, l4, l5, p0, p1, p2, p3, last, s0, *s1, *s2, *s3]
    spread = (
        (my_row, 8, x_col, LANES),
        (my_row, 8, z_col, r_cols),
        (my_row, 8, 0, wide),
        (core * r_half, r_half, 0, wide),
    )
    back = []
    for stage, (at, size, here) in enumerate(axes):
        sums[stage, here] = squares
        mine = sums.at[stage, here]
        group = [
            send(mine, mine, n_ssem.at[stage, j], n_rsem.at[stage, j], at(j)) for j in range(1, size)
        ]
        for copy in back:
            copy.wait_recv()
        row, height, col, width = spread[stage]
        part = rgrad.at[pl.ds(pl.multiple_of(row, 8), height), pl.ds(pl.multiple_of(col, LANES), width)]
        back = [
            send(part, part, r_ssem.at[4 + stage, j], r_rsem.at[4 + stage, j], at(j)) for j in range(1, size)
        ]
        waits += group + back
        for copy in group:
            copy.wait_recv()
        squares = sums[stage, 0]
        for k in range(1, size):
            squares = squares + sums[stage, k]
    total[...] = jnp.broadcast_to(jnp.sum(squares), total.shape)
    for copy in back:
        copy.wait_recv()
    for copy in waits:
        copy.wait_send()


def adam_update(gradient, moment_one, moment_two, weights):
    first_new = beta_first * moment_one + (1.0 - beta_first) * gradient
    second_new = beta_second * moment_two + (1.0 - beta_second) * gradient * gradient
    ratio = first_new / correct_first / (jnp.sqrt(second_new / correct_second) + adam_eps)
    weights_new = weights - learn_rate * (ratio + decay_weight * weights)
    return (weights_new, first_new, second_new)


def each(act, start=1):
    def step(j, carry):
        act(j)
        return carry

    lax.fori_loop(start, GROUPS, step, 0)


def move_kernel(
    limit,
    grad,
    total,
    master,
    first,
    second,
    partner,
    weight,
    new_master,
    new_first,
    new_second,
    leaving,
    middle0,
    middle1,
    middle2,
    turned,
    landed,
    ssem,
    rsem,
    a_ssem,
    a_rsem,
):
    zl, x, e = (lax.axis_index(a) for a in ALL)
    rows, wide = grad.shape
    half = wide // 2
    results = (new_master, new_first, new_second)
    middle = (middle0, middle1, middle2)

    def peer(j):
        return {"e": (e + j) % GROUPS}

    def at_x(j):
        return {"x": (x + j) % 4}

    pair = {"zl": 1 - zl}

    barrier = pltpu.get_barrier_semaphore()
    each(lambda j: pl.semaphore_signal(barrier, inc=1, device_id=peer(j), device_id_type=MESH))
    for device in (at_x(1), at_x(3), pair):
        pl.semaphore_signal(barrier, inc=1, device_id=device, device_id_type=MESH)

    factor = jnp.minimum(1.0, limit / (jnp.sqrt(total[0:1, 0:1]) + norm_eps))

    def columns(g):
        return pl.ds(pl.multiple_of(g * LANES, LANES), LANES)

    def update(g):
        c = columns(g)
        return adam_update(factor * grad[:, c], first[:, c], second[:, c], master[:, c])

    def encode(k, g, values):
        code = code_of(jnp.max(jnp.abs(values), axis=0, keepdims=True))
        leaving[k, g, 0:rows, :] = to_codes(values, code)
        leaving[k, g, rows:, :] = jnp.broadcast_to(code, (16, LANES)).astype(I16)

    def decode(k, g):
        piece = landed.at[k, g]
        values = piece[0:rows, :].astype(F32) * scale_of(piece[rows : rows + 1, :].astype(F32))
        results[k][:, columns(g)] = values
        return values

    def remote(src, dst, phase, k, j):
        return pltpu.make_async_remote_copy(
            src_ref=src,
            dst_ref=dst,
            send_sem=ssem.at[phase, k, j],
            recv_sem=rsem.at[phase, k, j],
            device_id=peer(j),
            device_id_type=MESH,
        )

    def go(k, j):
        return remote(leaving.at[k, (e + j) % GROUPS], middle[k].at[j], 0, k, j)

    def come(k, j):
        return remote(turned.at[k, (e + j) % GROUPS], landed.at[k, e], 1, k, j)

    def permute(k):
        middle[k][0] = leaving[k, e]

        def step(p, carry):
            turned[k, p] = middle[k][(e - partner[p] + GROUPS) % GROUPS]
            return carry

        lax.fori_loop(0, GROUPS, step, 0)

    def turn(k):
        each(lambda j: go(k, j).wait_recv())
        permute(k)
        each(lambda j: come(k, j).start())
        landed[k, e] = turned[k, e]

    encode(0, e, update(e)[0])
    pl.semaphore_wait(barrier, GROUPS + 2)

    def first_leg(j):
        g = (e + j) % GROUPS
        encode(0, g, update(g)[0])
        go(0, j).start()

    each(first_leg)

    def moments(g):
        _, first_new, second_new = update(g)
        encode(1, g, first_new)
        encode(2, g, second_new)

    each(moments, 0)
    turn(0)

    def weight_part(block, col, width):
        return weight.at[
            pl.ds(pl.multiple_of(block * rows, 16), rows), pl.ds(pl.multiple_of(col, LANES), width)
        ]

    own, twin = zl * 4 + x, (1 - zl) * 4 + x
    own_rows = pl.ds(pl.multiple_of(own * rows, 16), rows)

    def settle(g):
        weight[own_rows, columns(g)] = decode(0, g).astype(jnp.bfloat16)

    settle(e)

    def settle_next(j):
        come(0, j).wait_recv()
        settle((e - j + GROUPS) % GROUPS)

    each(settle_next)

    def gather(n, block, col, width, device):
        part = weight_part(block, col, width)
        return send(part, part, a_ssem.at[n], a_rsem.at[n], device)

    left, right = (x + 3) % 4, (x + 1) % 4
    g_pair = gather(0, own, 0, wide, pair)
    g_right = gather(1, own, 0, wide, at_x(1))
    g_left = gather(2, own, 0, wide, at_x(3))
    each(lambda j: go(1, j).start())
    each(lambda j: go(2, j).start())

    g_pair.wait_recv()
    t_right = gather(3, twin, 0, wide, at_x(1))
    t_left = gather(4, twin, 0, wide, at_x(3))
    g_right.wait_recv()
    f_right = gather(5, zl * 4 + left, 0, half, at_x(1))
    g_left.wait_recv()
    f_left = gather(6, zl * 4 + right, half, half, at_x(3))

    turn(1)
    t_right.wait_recv()
    h_right = gather(7, (1 - zl) * 4 + left, 0, half, at_x(1))
    t_left.wait_recv()
    h_left = gather(8, (1 - zl) * 4 + right, half, half, at_x(3))
    turn(2)

    for k in (1, 2):
        decode(k, e)

        def finish(j, k=k):
            come(k, j).wait_recv()
            decode(k, (e - j + GROUPS) % GROUPS)

        each(finish)
    for copy in (f_right, f_left, h_right, h_left):
        copy.wait_recv()
    for k in range(3):
        each(lambda j, k=k: go(k, j).wait_send())
        each(lambda j, k=k: come(k, j).wait_send())
    for copy in (g_pair, g_right, g_left, t_right, t_left, f_right, f_left, h_right, h_left):
        copy.wait_send()


def on_device(
    hidden,
    upstream,
    token_counts,
    master,
    first_moment,
    second_moment,
    router_input,
    router_cot,
    router_master,
    router_first,
    router_second,
    partner,
):
    depth, units = hidden.shape[1:]
    wide = upstream.shape[2]
    rows = units // 8
    n_router = router_cot.shape[0]
    vmem = pl.BlockSpec(memory_space=pltpu.VMEM)
    smem = pl.BlockSpec(memory_space=pltpu.SMEM)
    dma = pltpu.SemaphoreType.DMA
    coded = wide + LANES
    r_half, r_cols = n_router // 2, wide // 4
    late = rows * 5 // 11 // 16 * 16
    early = rows - late
    late_a = (late // 16 + 1) // 2 * 16
    gradient, router_grad, total = pl.pallas_call(
        reduce_kernel,
        out_shape=(
            jax.ShapeDtypeStruct((rows, wide), F32),
            jax.ShapeDtypeStruct((n_router, wide), F32),
            jax.ShapeDtypeStruct((8, LANES), F32),
        ),
        in_specs=[vmem, vmem, smem, vmem, vmem],
        out_specs=(vmem, vmem, vmem),
        scratch_shapes=[
            pltpu.VMEM((units, depth), jnp.bfloat16),
            pltpu.VMEM((8, rows, wide), F32),
            *[pltpu.VMEM((6, early, coded), I16)] * 2,
            *[pltpu.VMEM((6, late_a, coded), I16)] * 2,
            *[pltpu.VMEM((4, late, coded), I16)] * 2,
            *[pltpu.VMEM((early, coded), I16)] * 2,
            pltpu.VMEM((n_router, wide), F32),
            pltpu.VMEM((r_half, wide), F32),
            pltpu.VMEM((r_half, wide), F32),
            pltpu.VMEM((3, 8, wide), F32),
            pltpu.VMEM((8, wide), F32),
            pltpu.VMEM((3, 8, r_cols), F32),
            pltpu.VMEM((8, r_cols), F32),
            pltpu.VMEM((3, 8, LANES), F32),
            pltpu.VMEM((4, 4, 8, LANES), F32),
            dma((12,)),
            dma((12,)),
            dma((5,)),
            dma((5,)),
            dma((8, 4)),
            dma((8, 4)),
            dma((4, 4)),
            dma((4, 4)),
        ],
        compiler_params=pltpu.CompilerParams(
            collective_id=0, has_side_effects=True, vmem_limit_bytes=40 * 1024 * 1024
        ),
        name="reduce",
    )(hidden[0], upstream[0], token_counts, router_cot, router_input)

    clip_limit = 2.0 * math.sqrt(float(GROUPS * units * wide + n_router * wide))
    tall = rows + 16
    state = jax.ShapeDtypeStruct((rows, wide), F32)
    weight, new_master, new_first, new_second = pl.pallas_call(
        functools.partial(move_kernel, clip_limit),
        out_shape=(jax.ShapeDtypeStruct((units, wide), jnp.bfloat16), state, state, state),
        in_specs=[vmem, vmem, vmem, vmem, vmem, smem],
        out_specs=(vmem, vmem, vmem, vmem),
        scratch_shapes=[
            pltpu.VMEM((3, GROUPS, tall, LANES), I16),
            *[pltpu.VMEM((GROUPS, tall, LANES), I16)] * 3,
            *[pltpu.VMEM((3, GROUPS, tall, LANES), I16)] * 2,
            dma((2, 3, GROUPS)),
            dma((2, 3, GROUPS)),
            dma((9,)),
            dma((9,)),
        ],
        compiler_params=pltpu.CompilerParams(
            collective_id=1, has_side_effects=True, vmem_limit_bytes=27 * 1024 * 1024
        ),
        name="move",
    )(gradient, total, master[0], first_moment[0], second_moment[0], partner)

    factor = jnp.minimum(1.0, clip_limit / (jnp.sqrt(total[0, 0]) + norm_eps))
    router_outs = adam_update(factor * router_grad, router_first, router_second, router_master)

    return (
        weight[None],
        new_master[None],
        new_first[None],
        new_second[None],
        router_outs[0],
        router_outs[1],
        router_outs[2],
    )


def solution(mesh):
    split = Mesh(mesh.devices.reshape(2, 4, mesh.shape["expert"]), ALL)
    return jax.shard_map(
        on_device,
        mesh=split,
        in_specs=(
            P("e", DP, None),
            P("e", DP, None),
            P("e", DP),
            P("e", DP, None),
            P("e", DP, None),
            P("e", DP, None),
            P(ALL, None),
            P(None, ALL),
            P(),
            P(),
            P(),
            P(),
        ),
        out_specs=(
            P("e", None, None),
            P("e", DP, None),
            P("e", DP, None),
            P("e", DP, None),
            P(),
            P(),
            P(),
        ),
        check_vma=False,
    )
```

```python
import functools
import math

import jax
import jax.numpy as jnp
from jax import lax
from jax.experimental import pallas as pl
from jax.experimental.pallas import tpu as pltpu
from jax.sharding import Mesh
from jax.sharding import PartitionSpec as P

MESH = pl.DeviceIdType.MESH
DP = ("zl", "x")
ALL = ("zl", "x", "e")
F32 = jnp.float32
I16 = jnp.int16

beta_first = 0.9
beta_second = 0.95
learn_rate = 0.001
decay_weight = 0.1
adam_eps = 1e-08
norm_eps = 1e-06
correct_first = 1.0 - 0.9**10
correct_second = 1.0 - 0.95**10

GROUPS = 16
LANES = 128
TOP = 15.0
SMALL = 2.0**-100


def code_of(peak):
    return jnp.ceil(16.0 * jnp.log2(jnp.maximum(peak, SMALL)))


def to_codes(values, code):
    scaled = jnp.round(values * jnp.exp2(TOP - code * (1.0 / 16.0)))
    return jnp.clip(scaled, -32767.0, 32767.0).astype(I16)


def scale_of(code):
    return jnp.exp2(code * (1.0 / 16.0) - TOP)


def encode_rows(values, dst, rows):
    width = values.shape[1]
    code = code_of(jnp.max(jnp.abs(values), axis=1, keepdims=True))
    dst[rows, :width] = to_codes(values, code)
    dst[rows, width:] = jnp.broadcast_to(code, (values.shape[0], LANES)).astype(I16)


def decode_rows(src, rows, width):
    code = src[rows, width : width + LANES].astype(F32)[:, :1]
    return src[rows, :width].astype(F32) * scale_of(code)


def send(src, dst, send_sem, recv_sem, device):
    copy = pltpu.make_async_remote_copy(
        src_ref=src, dst_ref=dst, send_sem=send_sem, recv_sem=recv_sem, device_id=device, device_id_type=MESH
    )
    copy.start()
    return copy


def reduce_kernel(
    hid_hbm,
    up_hbm,
    counts,
    cot_hbm,
    rin_hbm,
    grad,
    rgrad,
    total,
    hid,
    up,
    cot,
    rin,
    hid_t,
    terms,
    x_out,
    x_in,
    late_out,
    late_in,
    z_out,
    z_in,
    last_out,
    last_in,
    rp,
    r_in0,
    r1,
    r_in1,
    r2,
    r_in2,
    r3,
    r_in3,
    piece,
    plane_sums,
    side_sums,
    load_sem,
    x_ssem,
    x_rsem,
    z_ssem,
    z_rsem,
    r_ssem,
    r_rsem,
    n_ssem,
    n_rsem,
):
    zl, x, e = (lax.axis_index(a) for a in ALL)
    y, zh, core = e // 4, (e // 2) % 2, e % 2
    z = zh * 2 + zl
    depth, units = hid.shape
    wide = up.shape[1]
    rows = units // 8
    early = x_out.shape[1]
    late = rows - early
    late_a = late_out.shape[1]
    late_b = late - late_a

    def at_x(j):
        return {"x": (x + j) % 4}

    def at_z(j):
        there = (z + j) % 4
        return {"zl": there % 2, "e": y * 4 + (there // 2) * 2 + core}

    def at_y(j):
        return {"e": ((y + j) % 4) * 4 + zh * 2 + core}

    def at_core(j):
        return {"e": e + 1 - 2 * core}

    pair = {"zl": 1 - zl}

    def at_plane(j):
        there = (z + j % 4) % 4
        return {"x": (x + j // 4) % 4, "zl": there % 2, "e": y * 4 + (there // 2) * 2 + core}

    def at_side(j):
        return {"e": ((y + j // 2) % 4) * 4 + zh * 2 + (core + j) % 2}

    loads = [
        pltpu.make_async_copy(src, dst, load_sem.at[n])
        for n, (src, dst) in enumerate(((hid_hbm, hid), (up_hbm, up), (cot_hbm, cot), (rin_hbm, rin)))
    ]
    for copy in loads:
        copy.start()
    barrier = pltpu.get_barrier_semaphore()
    for at, size in ((at_plane, 16), (at_side, 8)):
        for j in range(1, size):
            pl.semaphore_signal(barrier, inc=1, device_id=at(j), device_id_type=MESH)

    live = counts[0, 0]
    keep = (lax.broadcasted_iota(jnp.int32, (depth, LANES), 0) < live).astype(F32).astype(jnp.bfloat16)
    loads[0].wait()

    @pl.loop(0, units // LANES)
    def _(t):
        cols = pl.ds(pl.multiple_of(t * LANES, LANES), LANES)
        hid_t[cols, :] = (hid[:, cols] * keep).T

    def multiply(block):
        at = pl.multiple_of(block * rows, 16)

        @pl.loop(0, wide // 512)
        def _(n):
            cols = pl.ds(pl.multiple_of(n * 512, 512), 512)
            terms[block, :, cols] = jnp.dot(hid_t[pl.ds(at, rows), :], up[:, cols], preferred_element_type=F32)

    def tiles(start, size, act):
        @pl.loop(0, size // 16, unroll=True)
        def _(i):
            act(
                pl.ds(pl.multiple_of(start + i * 16, 16), 16),
                pl.ds(pl.multiple_of(i * 16, 16), 16),
            )

    def x_copy(slot, device):
        return send(x_out.at[slot], x_in.at[slot], x_ssem.at[slot], x_rsem.at[slot], device)

    def late_copy(slot, size, device):
        r = pl.ds(0, size)
        return send(
            late_out.at[slot, r], late_in.at[slot, r], x_ssem.at[6 + slot], x_rsem.at[6 + slot], device
        )

    def early_part(block, slot, step, incoming=None):
        def act(r, i):
            values = terms[block, r, :]
            if incoming is not None:
                values = values + decode_rows(x_in.at[incoming], i, wide)
            encode_rows(values, x_out.at[slot], i)

        tiles(0, early, act)
        return x_copy(slot, at_x(step))

    def pair_part(n, there):
        def act(r, i):
            encode_rows(terms[(1 - zl) * 4 + there, r, :], z_out.at[n], i)

        tiles(early, late, act)
        return send(z_out.at[n], z_in.at[n], z_ssem.at[n], z_rsem.at[n], pair)

    def pair_sum(n, there):
        block = zl * 4 + there

        def act(r, i):
            terms[block, r, :] += decode_rows(z_in.at[n], i, wide)

        tiles(early, late, act)

    def late_part(there, start, size, slot, step, incoming=None):
        block = zl * 4 + there

        def act(r, i):
            values = terms[block, r, :]
            if incoming is not None:
                values = values + decode_rows(late_in.at[incoming], i, wide)
            encode_rows(values, late_out.at[slot], i)

        tiles(start, size, act)
        return late_copy(slot, size, at_x(step))

    far, right, left = (x + 2) % 4, (x + 1) % 4, (x + 3) % 4
    a_at, b_at = early, early + late_a

    loads[1].wait()
    multiply(far)
    pl.semaphore_wait(barrier, 22)
    e0 = early_part(far, 0, 3)
    multiply(4 + far)
    e1 = early_part(4 + far, 1, 1)
    p0 = pair_part(0, far)
    multiply(right)
    e2 = early_part(right, 2, 1)
    multiply(4 + left)
    e3 = early_part(4 + left, 3, 3)
    multiply(4 + right)
    p1 = pair_part(1, right)

    loads[2].wait()
    loads[3].wait()
    rp[...] = jnp.dot(cot[...], rin[...], preferred_element_type=F32)
    n_router = rp.shape[0]
    r_half, r_cols = n_router // 2, wide // 4
    s0 = send(
        rp.at[pl.ds(pl.multiple_of((1 - core) * r_half, 8), r_half)],
        r_in0,
        r_ssem.at[0, 1],
        r_rsem.at[0, 1],
        at_core(1),
    )
    multiply(left)
    p2 = pair_part(2, left)
    s0.wait_recv()
    r1[...] = rp[pl.ds(pl.multiple_of(core * r_half, 8), r_half), :] + r_in0[...]
    s1 = [
        send(
            r1.at[pl.ds(pl.multiple_of(((y + j) % 4) * 8, 8), 8)],
            r_in1.at[j - 1],
            r_ssem.at[1, j],
            r_rsem.at[1, j],
            at_y(j),
        )
        for j in range(1, 4)
    ]
    multiply(x)
    multiply(4 + x)
    p3 = pair_part(3, x)

    e0.wait_recv()
    e4 = early_part(left, 4, 3, 0)
    e1.wait_recv()
    e5 = early_part(4 + right, 5, 1, 1)
    p0.wait_recv()
    pair_sum(0, far)
    l0 = late_part(far, a_at, late_a, 0, 3)
    l1 = late_part(far, b_at, late_b, 1, 1)

    for copy in s1:
        copy.wait_recv()
    r2[...] = r1[pl.ds(pl.multiple_of(y * 8, 8), 8), :] + r_in1[0] + r_in1[1] + r_in1[2]
    s2 = [
        send(
            r2.at[:, pl.ds(pl.multiple_of(((z + j) % 4) * r_cols, LANES), r_cols)],
            r_in2.at[j - 1],
            r_ssem.at[2, j],
            r_rsem.at[2, j],
            at_z(j),
        )
        for j in range(1, 4)
    ]
    p1.wait_recv()
    pair_sum(1, right)
    l2 = late_part(right, a_at, late_a, 2, 1)
    for copy in s2:
        copy.wait_recv()
    r3[...] = r2[:, pl.ds(pl.multiple_of(z * r_cols, LANES), r_cols)] + r_in2[0] + r_in2[1] + r_in2[2]
    s3 = [
        send(
            r3.at[:, pl.ds(pl.multiple_of(((x + j) % 4) * LANES, LANES), LANES)],
            r_in3.at[j - 1],
            r_ssem.at[3, j],
            r_rsem.at[3, j],
            at_x(j),
        )
        for j in range(1, 4)
    ]
    p2.wait_recv()
    pair_sum(2, left)
    l3 = late_part(left, b_at, late_b, 3, 3)

    for copy in (e2, e3, e4, e5):
        copy.wait_recv()

    def fold(r, i):
        terms[x, r, :] += decode_rows(x_in.at[2], i, wide) + decode_rows(x_in.at[4], i, wide)
        terms[4 + x, r, :] += decode_rows(x_in.at[3], i, wide) + decode_rows(x_in.at[5], i, wide)
        encode_rows(terms[(1 - zl) * 4 + x, r, :], last_out, i)

    tiles(0, early, fold)
    last = send(last_out, last_in, z_ssem.at[4], z_rsem.at[4], pair)
    for copy in s3:
        copy.wait_recv()
    piece[...] = r3[:, pl.ds(pl.multiple_of(x * LANES, LANES), LANES)] + r_in3[0] + r_in3[1] + r_in3[2]
    my_row = core * r_half + y * 8
    z_col = z * r_cols
    x_col = z_col + x * LANES
    rgrad[pl.ds(pl.multiple_of(my_row, 8), 8), pl.ds(pl.multiple_of(x_col, LANES), LANES)] = piece[...]

    def give_back(stage, row, height, col, width, at, size):
        part = rgrad.at[pl.ds(pl.multiple_of(row, 8), height), pl.ds(pl.multiple_of(col, LANES), width)]
        return [
            send(part, part, r_ssem.at[stage, j], r_rsem.at[stage, j], at(j)) for j in range(1, size)
        ]

    b0 = give_back(4, my_row, 8, x_col, LANES, at_x, 4)


    l0.wait_recv()
    l4 = late_part(left, a_at, late_a, 4, 3, 0)
    l1.wait_recv()
    l5 = late_part(right, b_at, late_b, 5, 1, 1)
    p3.wait_recv()
    pair_sum(3, x)
    for copy in b0:
        copy.wait_recv()
    b1 = give_back(5, my_row, 8, z_col, r_cols, at_z, 4)

    own = zl * 4 + x

    def count(values, acc):
        values = values * values
        for a in range(2):
            for b in range(wide // LANES):
                acc = acc + values[a * 8 : a * 8 + 8, b * LANES : (b + 1) * LANES]
        return acc

    def close(start, size, acc, sources):
        def step(n, acc):
            i = pl.ds(pl.multiple_of(n * 16, 16), 16)
            r = pl.ds(pl.multiple_of(start + n * 16, 16), 16)
            values = terms[own, r, :]
            for source in sources:
                values = values + decode_rows(source, i, wide)
            grad[r, :] = values
            return count(values, acc)

        return lax.fori_loop(0, size // 16, step, acc, unroll=True)

    squares = jnp.zeros((8, LANES), F32)
    last.wait_recv()
    squares = close(0, early, squares, (last_in,))
    for copy in b1:
        copy.wait_recv()
    b2 = give_back(6, my_row, 8, 0, wide, at_y, 4)
    for copy in (l2, l4):
        copy.wait_recv()
    squares = close(a_at, late_a, squares, (late_in.at[2], late_in.at[4]))
    for copy in (l3, l5):
        copy.wait_recv()
    squares = close(b_at, late_b, squares, (late_in.at[3], late_in.at[5]))

    squares = squares + piece[...] * piece[...]

    def tell(buf, here, at, size, sem):
        buf[here] = squares
        mine = buf.at[here]
        return [send(mine, mine, n_ssem.at[sem + j], n_rsem.at[sem + j], at(j)) for j in range(1, size)]

    def sum_of(buf, size, group):
        for copy in group:
            copy.wait_recv()
        acc = buf[0]
        for k in range(1, size):
            acc = acc + buf[k]
        return acc

    plane_copies = tell(plane_sums, x * 4 + z, at_plane, 16, 0)
    for copy in b2:
        copy.wait_recv()
    b3 = give_back(7, core * r_half, r_half, 0, wide, at_core, 2)
    squares = sum_of(plane_sums, 16, plane_copies)
    side_copies = tell(side_sums, y * 2 + core, at_side, 8, 16)
    squares = sum_of(side_sums, 8, side_copies)
    total[...] = jnp.broadcast_to(jnp.sum(squares), total.shape)
    for copy in b3:
        copy.wait_recv()
    waits = [e0, e1, e2, e3, e4, e5, l0, l1, l2, l3, l4, l5, p0, p1, p2, p3, last, s0, *s1, *s2, *s3]
    for copy in waits + b0 + b1 + b2 + b3 + plane_copies + side_copies:
        copy.wait_send()


def adam_update(gradient, moment_one, moment_two, weights):
    first_new = beta_first * moment_one + (1.0 - beta_first) * gradient
    second_new = beta_second * moment_two + (1.0 - beta_second) * gradient * gradient
    ratio = first_new / correct_first / (jnp.sqrt(second_new / correct_second) + adam_eps)
    weights_new = weights - learn_rate * (ratio + decay_weight * weights)
    return (weights_new, first_new, second_new)


def in_hbm(array):
    return pltpu.with_memory_space_constraint(array, pltpu.HBM)


def each(act, start=1):
    def step(j, carry):
        act(j)
        return carry

    lax.fori_loop(start, GROUPS, step, 0)


def move_kernel(
    limit,
    grad,
    total,
    master,
    first,
    second,
    partner,
    weight,
    new_master,
    new_first,
    new_second,
    lead_out0,
    lead_out1,
    lead_mid0,
    lead_mid1,
    lead_turn0,
    lead_turn1,
    lead_land0,
    lead_land1,
    lead_twin0,
    lead_twin1,
    leaving,
    middle0,
    middle1,
    turned,
    landed,
    l_ssem,
    l_rsem,
    ssem,
    rsem,
    a_ssem,
    a_rsem,
):
    zl, x, e = (lax.axis_index(a) for a in ALL)
    rows, wide = grad.shape
    half = wide // 2
    results = (new_first, new_second)
    lead_out, lead_mid = (lead_out0, lead_out1), (lead_mid0, lead_mid1)
    lead_turn, lead_land, lead_twin = (lead_turn0, lead_turn1), (lead_land0, lead_land1), (lead_twin0, lead_twin1)
    middle = (middle0, middle1)
    split = lead_out0.shape[1] - 16
    runs = ((0, split), (split, rows - split))

    def peer(j):
        return {"e": (e + j) % GROUPS}

    def twin_peer(j):
        return {"e": (e + j) % GROUPS, "zl": 1 - zl}

    def at_x(j):
        return {"x": (x + j) % 4}

    barrier = pltpu.get_barrier_semaphore()
    each(lambda j: pl.semaphore_signal(barrier, inc=1, device_id=peer(j), device_id_type=MESH))
    each(lambda j: pl.semaphore_signal(barrier, inc=1, device_id=twin_peer(j), device_id_type=MESH), 0)
    for device in (at_x(1), at_x(3)):
        pl.semaphore_signal(barrier, inc=1, device_id=device, device_id_type=MESH)

    factor = jnp.minimum(1.0, limit / (jnp.sqrt(total[0:1, 0:1]) + norm_eps))

    def columns(g):
        return pl.ds(pl.multiple_of(g * LANES, LANES), LANES)

    def update(g, start=0, size=rows):
        c, r = columns(g), pl.ds(start, size)
        return adam_update(factor * grad[r, c], first[r, c], second[r, c], master[r, c])

    def pack(piece, size, values):
        code = code_of(jnp.max(jnp.abs(values), axis=0, keepdims=True))
        piece[0:size, :] = to_codes(values, code)
        piece[size:, :] = jnp.broadcast_to(code, (16, LANES)).astype(I16)

    def unpack(piece, size):
        return piece[0:size, :].astype(F32) * scale_of(piece[size : size + 1, :].astype(F32))

    def remote(src, dst, send_sem, recv_sem, device):
        return pltpu.make_async_remote_copy(
            src_ref=src,
            dst_ref=dst,
            send_sem=send_sem,
            recv_sem=recv_sem,
            device_id=device,
            device_id_type=MESH,
        )

    def lead_go(h, j):
        at = (0, h, j)
        return remote(lead_out[h].at[(e + j) % GROUPS], lead_mid[h].at[j], l_ssem.at[at], l_rsem.at[at], peer(j))

    def lead_come(h, j):
        at = (1, h, j)
        src = lead_turn[h].at[(e + j) % GROUPS]
        return remote(src, lead_land[h].at[e], l_ssem.at[at], l_rsem.at[at], peer(j))

    def lead_cross(h, j):
        at = (2, h, j)
        src = lead_turn[h].at[(e + j) % GROUPS]
        return remote(src, lead_twin[h].at[e], l_ssem.at[at], l_rsem.at[at], twin_peer(j))

    def go(k, j):
        at = (0, k, j)
        return remote(leaving.at[k, (e + j) % GROUPS], middle[k].at[j], ssem.at[at], rsem.at[at], peer(j))

    def come(k, j):
        at = (1, k, j)
        return remote(turned.at[k, (e + j) % GROUPS], landed.at[k, e], ssem.at[at], rsem.at[at], peer(j))

    def permute(arrived, to):
        def step(p, carry):
            to[p] = arrived[(e - partner[p] + GROUPS) % GROUPS]
            return carry

        lax.fori_loop(0, GROUPS, step, 0)

    for h, run in enumerate(runs):
        pack(lead_out[h].at[e], run[1], update(e, *run)[0])
    pl.semaphore_wait(barrier, 2 * GROUPS + 1)
    for h, run in enumerate(runs):

        def first_leg(j, h=h, run=run):
            g = (e + j) % GROUPS
            pack(lead_out[h].at[g], run[1], update(g, *run)[0])
            lead_go(h, j).start()

        each(first_leg)
        lead_mid[h][0] = lead_out[h][e]

    for h in range(2):
        each(lambda j, h=h: lead_go(h, j).wait_recv())
        permute(lead_mid[h], lead_turn[h])
        each(lambda j, h=h: lead_come(h, j).start())
        lead_land[h][e] = lead_turn[h][e]
    for h in range(2):
        each(lambda j, h=h: lead_cross(h, j).start(), 0)

    def moments(g):
        _, first_new, second_new = update(g)
        pack(leaving.at[0, g], rows, first_new)
        pack(leaving.at[1, g], rows, second_new)

    each(moments, 0)

    own, twin = zl * 4 + x, (1 - zl) * 4 + x
    left, right = (x + 3) % 4, (x + 1) % 4

    def weight_rows(block, h):
        return pl.ds(pl.multiple_of(block * rows + runs[h][0], 16), runs[h][1])

    def gather(n, h, block, col, width, device):
        part = weight.at[weight_rows(block, h), pl.ds(col, width)]
        return send(part, part, a_ssem.at[n, h], a_rsem.at[n, h], device)

    def settle(h, g):
        values = unpack(lead_land[h].at[g], runs[h][1])
        new_master[pl.ds(*runs[h]), columns(g)] = values
        weight[weight_rows(own, h), columns(g)] = values.astype(jnp.bfloat16)

    def settle_twin(h, g):
        values = unpack(lead_twin[h].at[g], runs[h][1])
        weight[weight_rows(twin, h), columns(g)] = values.astype(jnp.bfloat16)

    to_right, to_left = [], []
    for h in range(2):
        settle(h, e)

        def settle_next(j, h=h):
            lead_come(h, j).wait_recv()
            settle(h, (e - j + GROUPS) % GROUPS)

        each(settle_next)
        to_right.append(gather(0, h, own, 0, wide, at_x(1)))
        to_left.append(gather(1, h, own, 0, wide, at_x(3)))

    each(lambda j: go(0, j).start())
    each(lambda j: go(1, j).start())

    twin_right, twin_left = [], []
    for h in range(2):

        def settle_cross(j, h=h):
            lead_cross(h, j).wait_recv()
            settle_twin(h, (e - j + GROUPS) % GROUPS)

        each(settle_cross, 0)
        twin_right.append(gather(2, h, twin, 0, wide, at_x(1)))
        twin_left.append(gather(3, h, twin, 0, wide, at_x(3)))

    onward = []

    def pass_on(n, h, z_at, from_left, from_right):
        from_left.wait_recv()
        onward.append(gather(n, h, z_at * 4 + left, 0, half, at_x(1)))
        from_right.wait_recv()
        onward.append(gather(n + 1, h, z_at * 4 + right, half, half, at_x(3)))

    def turn(k):
        each(lambda j: go(k, j).wait_recv())
        middle[k][0] = leaving[k, e]
        permute(middle[k], turned.at[k])
        each(lambda j: come(k, j).start())
        landed[k, e] = turned[k, e]

    pass_on(4, 0, zl, to_right[0], to_left[0])
    pass_on(4, 1, zl, to_right[1], to_left[1])
    turn(0)
    pass_on(6, 0, 1 - zl, twin_right[0], twin_left[0])
    turn(1)
    pass_on(6, 1, 1 - zl, twin_right[1], twin_left[1])

    for k in range(2):

        def finish(g, k=k):
            results[k][:, columns(g)] = unpack(landed.at[k, g], rows)

        def finish_next(j, k=k, finish=finish):
            come(k, j).wait_recv()
            finish((e - j + GROUPS) % GROUPS)

        finish(e)
        each(finish_next)
    for copy in onward:
        copy.wait_recv()
    for k in range(2):
        each(lambda j, k=k: lead_go(k, j).wait_send())
        each(lambda j, k=k: lead_come(k, j).wait_send())
        each(lambda j, k=k: lead_cross(k, j).wait_send(), 0)
        each(lambda j, k=k: go(k, j).wait_send())
        each(lambda j, k=k: come(k, j).wait_send())
    for copy in to_right + to_left + twin_right + twin_left + onward:
        copy.wait_send()


def on_device(
    hidden,
    upstream,
    token_counts,
    master,
    first_moment,
    second_moment,
    router_input,
    router_cot,
    router_master,
    router_first,
    router_second,
    partner,
):
    depth, units = hidden.shape[1:]
    wide = upstream.shape[2]
    rows = units // 8
    n_router = router_cot.shape[0]
    vmem = pl.BlockSpec(memory_space=pltpu.VMEM)
    smem = pl.BlockSpec(memory_space=pltpu.SMEM)
    hbm = pl.BlockSpec(memory_space=pltpu.HBM)
    dma = pltpu.SemaphoreType.DMA
    coded = wide + LANES
    r_half, r_cols = n_router // 2, wide // 4
    late = rows * 5 // 11 // 16 * 16
    early = rows - late
    late_a = (late // 16 + 1) // 2 * 16
    gradient, router_grad, total = pl.pallas_call(
        reduce_kernel,
        out_shape=(
            jax.ShapeDtypeStruct((rows, wide), F32),
            jax.ShapeDtypeStruct((n_router, wide), F32),
            jax.ShapeDtypeStruct((8, LANES), F32),
        ),
        in_specs=[hbm, hbm, smem, hbm, hbm],
        out_specs=(vmem, vmem, vmem),
        scratch_shapes=[
            pltpu.VMEM((depth, units), jnp.bfloat16),
            pltpu.VMEM((depth, wide), jnp.bfloat16),
            pltpu.VMEM(router_cot.shape, jnp.bfloat16),
            pltpu.VMEM(router_input.shape, jnp.bfloat16),
            pltpu.VMEM((units, depth), jnp.bfloat16),
            pltpu.VMEM((8, rows, wide), F32),
            *[pltpu.VMEM((6, early, coded), I16)] * 2,
            *[pltpu.VMEM((6, late_a, coded), I16)] * 2,
            *[pltpu.VMEM((4, late, coded), I16)] * 2,
            *[pltpu.VMEM((early, coded), I16)] * 2,
            pltpu.VMEM((n_router, wide), F32),
            pltpu.VMEM((r_half, wide), F32),
            pltpu.VMEM((r_half, wide), F32),
            pltpu.VMEM((3, 8, wide), F32),
            pltpu.VMEM((8, wide), F32),
            pltpu.VMEM((3, 8, r_cols), F32),
            pltpu.VMEM((8, r_cols), F32),
            pltpu.VMEM((3, 8, LANES), F32),
            pltpu.VMEM((8, LANES), F32),
            pltpu.VMEM((16, 8, LANES), F32),
            pltpu.VMEM((8, 8, LANES), F32),
            dma((4,)),
            dma((12,)),
            dma((12,)),
            dma((5,)),
            dma((5,)),
            dma((8, 4)),
            dma((8, 4)),
            dma((24,)),
            dma((24,)),
        ],
        compiler_params=pltpu.CompilerParams(
            collective_id=0, has_side_effects=True, vmem_limit_bytes=40 * 1024 * 1024
        ),
        name="reduce",
    )(in_hbm(hidden[0]), in_hbm(upstream[0]), token_counts, in_hbm(router_cot), in_hbm(router_input))

    clip_limit = 2.0 * math.sqrt(float(GROUPS * units * wide + n_router * wide))
    tall = rows + 16
    split = (rows // 16 + 1) // 2 * 16
    state = jax.ShapeDtypeStruct((rows, wide), F32)
    weight, new_master, new_first, new_second = pl.pallas_call(
        functools.partial(move_kernel, clip_limit),
        out_shape=(jax.ShapeDtypeStruct((units, wide), jnp.bfloat16), state, state, state),
        in_specs=[vmem, vmem, vmem, vmem, vmem, smem],
        out_specs=(vmem, vmem, vmem, vmem),
        scratch_shapes=[
            *[pltpu.VMEM((GROUPS, n, LANES), I16) for n in (split + 16, rows - split + 16)] * 5,
            pltpu.VMEM((2, GROUPS, tall, LANES), I16),
            *[pltpu.VMEM((GROUPS, tall, LANES), I16)] * 2,
            *[pltpu.VMEM((2, GROUPS, tall, LANES), I16)] * 2,
            dma((3, 2, GROUPS)),
            dma((3, 2, GROUPS)),
            dma((2, 2, GROUPS)),
            dma((2, 2, GROUPS)),
            dma((8, 2)),
            dma((8, 2)),
        ],
        compiler_params=pltpu.CompilerParams(
            collective_id=1, has_side_effects=True, vmem_limit_bytes=27 * 1024 * 1024
        ),
        name="move",
    )(gradient, total, master[0], first_moment[0], second_moment[0], partner)

    factor = jnp.minimum(1.0, clip_limit / (jnp.sqrt(total[0, 0]) + norm_eps))
    router_outs = adam_update(factor * router_grad, router_first, router_second, router_master)

    return (
        weight[None],
        new_master[None],
        new_first[None],
        new_second[None],
        router_outs[0],
        router_outs[1],
        router_outs[2],
    )


def solution(mesh):
    split = Mesh(mesh.devices.reshape(2, 4, mesh.shape["expert"]), ALL)
    return jax.shard_map(
        on_device,
        mesh=split,
        in_specs=(
            P("e", DP, None),
            P("e", DP, None),
            P("e", DP),
            P("e", DP, None),
            P("e", DP, None),
            P("e", DP, None),
            P(ALL, None),
            P(None, ALL),
            P(),
            P(),
            P(),
            P(),
        ),
        out_specs=(
            P("e", None, None),
            P("e", DP, None),
            P("e", DP, None),
            P("e", DP, None),
            P(),
            P(),
            P(),
        ),
        check_vma=False,
    )
```

```python
import functools
import math

import jax
import jax.numpy as jnp
from jax import lax
from jax.experimental import pallas as pl
from jax.experimental.pallas import tpu as pltpu
from jax.sharding import Mesh
from jax.sharding import PartitionSpec as P

MESH = pl.DeviceIdType.MESH
DP = ("zl", "x")
ALL = ("zl", "x", "e")
F32 = jnp.float32
I16 = jnp.int16

beta_first = 0.9
beta_second = 0.95
learn_rate = 0.001
decay_weight = 0.1
adam_eps = 1e-08
norm_eps = 1e-06
correct_first = 1.0 - 0.9**10
correct_second = 1.0 - 0.95**10

GROUPS = 16
LANES = 128
TOP = 15.0
SMALL = 2.0**-100


def code_of(peak):
    return jnp.ceil(16.0 * jnp.log2(jnp.maximum(peak, SMALL)))


def to_codes(values, code):
    scaled = jnp.round(values * jnp.exp2(TOP - code * (1.0 / 16.0)))
    return jnp.clip(scaled, -32767.0, 32767.0).astype(I16)


def scale_of(code):
    return jnp.exp2(code * (1.0 / 16.0) - TOP)


def encode_rows(values, dst, rows):
    width = values.shape[1]
    code = code_of(jnp.max(jnp.abs(values), axis=1, keepdims=True))
    dst[rows, :width] = to_codes(values, code)
    dst[rows, width:] = jnp.broadcast_to(code, (values.shape[0], LANES)).astype(I16)


def decode_rows(src, rows, width):
    code = src[rows, width : width + LANES].astype(F32)[:, :1]
    return src[rows, :width].astype(F32) * scale_of(code)


def send(src, dst, send_sem, recv_sem, device):
    copy = pltpu.make_async_remote_copy(
        src_ref=src, dst_ref=dst, send_sem=send_sem, recv_sem=recv_sem, device_id=device, device_id_type=MESH
    )
    copy.start()
    return copy


def reduce_kernel(
    hid_hbm,
    up_hbm,
    counts,
    cot_hbm,
    rin_hbm,
    grad,
    rgrad,
    total,
    hid,
    up,
    cot,
    rin,
    hid_t,
    terms,
    x_out,
    x_in,
    late_out,
    late_in,
    z_out,
    z_in,
    last_out,
    last_in,
    rp,
    r_in0,
    r1,
    r_in1,
    r2,
    r_in2,
    r3,
    r_in3,
    piece,
    plane_sums,
    side_sums,
    load_sem,
    x_ssem,
    x_rsem,
    z_ssem,
    z_rsem,
    r_ssem,
    r_rsem,
    n_ssem,
    n_rsem,
):
    zl, x, e = (lax.axis_index(a) for a in ALL)
    y, zh, core = e // 4, (e // 2) % 2, e % 2
    z = zh * 2 + zl
    depth, units = hid.shape
    wide = up.shape[1]
    rows = units // 8
    early = x_out.shape[1]
    late = rows - early
    late_a = late_out.shape[1]
    late_b = late - late_a

    def at_x(j):
        return {"x": (x + j) % 4}

    def at_z(j):
        there = (z + j) % 4
        return {"zl": there % 2, "e": y * 4 + (there // 2) * 2 + core}

    def at_y(j):
        return {"e": ((y + j) % 4) * 4 + zh * 2 + core}

    def at_core(j):
        return {"e": e + 1 - 2 * core}

    pair = {"zl": 1 - zl}

    def at_plane(j):
        there = (z + j % 4) % 4
        return {"x": (x + j // 4) % 4, "zl": there % 2, "e": y * 4 + (there // 2) * 2 + core}

    def at_side(j):
        return {"e": ((y + j // 2) % 4) * 4 + zh * 2 + (core + j) % 2}

    loads = [
        pltpu.make_async_copy(src, dst, load_sem.at[n])
        for n, (src, dst) in enumerate(((hid_hbm, hid), (up_hbm, up), (cot_hbm, cot), (rin_hbm, rin)))
    ]
    for copy in loads:
        copy.start()
    barrier = pltpu.get_barrier_semaphore()
    for at, size in ((at_plane, 16), (at_side, 8)):
        for j in range(1, size):
            pl.semaphore_signal(barrier, inc=1, device_id=at(j), device_id_type=MESH)

    live = counts[0, 0]
    keep = (lax.broadcasted_iota(jnp.int32, (depth, LANES), 0) < live).astype(F32).astype(jnp.bfloat16)
    loads[0].wait()

    @pl.loop(0, units // LANES)
    def _(t):
        cols = pl.ds(pl.multiple_of(t * LANES, LANES), LANES)
        hid_t[cols, :] = (hid[:, cols] * keep).T

    def multiply(block):
        at = pl.multiple_of(block * rows, 16)

        @pl.loop(0, wide // 512)
        def _(n):
            cols = pl.ds(pl.multiple_of(n * 512, 512), 512)
            terms[block, :, cols] = jnp.dot(hid_t[pl.ds(at, rows), :], up[:, cols], preferred_element_type=F32)

    def tiles(start, size, act):
        @pl.loop(0, size // 16, unroll=True)
        def _(i):
            act(
                pl.ds(pl.multiple_of(start + i * 16, 16), 16),
                pl.ds(pl.multiple_of(i * 16, 16), 16),
            )

    def x_made(slot, device):
        return pltpu.make_async_remote_copy(
            src_ref=x_out.at[slot],
            dst_ref=x_in.at[slot],
            send_sem=x_ssem.at[slot],
            recv_sem=x_rsem.at[slot],
            device_id=device,
            device_id_type=MESH,
        )

    def x_copy(slot, device):
        copy = x_made(slot, device)
        copy.start()
        return copy

    def late_copy(slot, size, device):
        r = pl.ds(0, size)
        return send(
            late_out.at[slot, r], late_in.at[slot, r], x_ssem.at[6 + slot], x_rsem.at[6 + slot], device
        )

    def early_part(block, slot, step, incoming=None):
        def act(r, i):
            values = terms[block, r, :]
            if incoming is not None:
                values = values + decode_rows(x_in.at[incoming], i, wide)
            encode_rows(values, x_out.at[slot], i)

        tiles(0, early, act)
        return x_copy(slot, at_x(step))

    def pair_part(n, there):
        def act(r, i):
            encode_rows(terms[(1 - zl) * 4 + there, r, :], z_out.at[n], i)

        tiles(early, late, act)
        return send(z_out.at[n], z_in.at[n], z_ssem.at[n], z_rsem.at[n], pair)

    def pair_sum(n, there):
        block = zl * 4 + there

        def act(r, i):
            terms[block, r, :] += decode_rows(z_in.at[n], i, wide)

        tiles(early, late, act)

    def late_part(there, start, size, slot, step, incoming=None):
        block = zl * 4 + there

        def act(r, i):
            values = terms[block, r, :]
            if incoming is not None:
                values = values + decode_rows(late_in.at[incoming], i, wide)
            encode_rows(values, late_out.at[slot], i)

        tiles(start, size, act)
        return late_copy(slot, size, at_x(step))

    far, right, left = (x + 2) % 4, (x + 1) % 4, (x + 3) % 4
    a_at, b_at = early, early + late_a

    loads[1].wait()
    multiply((1 - zl) * 4 + far)
    pl.semaphore_wait(barrier, 22)
    p0 = pair_part(0, far)
    early_part((1 - zl) * 4 + far, 1 - zl, 1 + 2 * zl)
    multiply(zl * 4 + far)
    early_part(zl * 4 + far, zl, 3 - 2 * zl)
    e0, e1 = x_made(0, at_x(3)), x_made(1, at_x(1))
    multiply(right)
    e2 = early_part(right, 2, 1)
    multiply(4 + left)
    e3 = early_part(4 + left, 3, 3)
    multiply(4 + right)
    p1 = pair_part(1, right)

    loads[2].wait()
    loads[3].wait()
    rp[...] = jnp.dot(cot[...], rin[...], preferred_element_type=F32)
    n_router = rp.shape[0]
    r_half, r_cols = n_router // 2, wide // 4
    s0 = send(
        rp.at[pl.ds(pl.multiple_of((1 - core) * r_half, 8), r_half)],
        r_in0,
        r_ssem.at[0, 1],
        r_rsem.at[0, 1],
        at_core(1),
    )
    multiply(left)
    p2 = pair_part(2, left)
    s0.wait_recv()
    r1[...] = rp[pl.ds(pl.multiple_of(core * r_half, 8), r_half), :] + r_in0[...]
    s1 = [
        send(
            r1.at[pl.ds(pl.multiple_of(((y + j) % 4) * 8, 8), 8)],
            r_in1.at[j - 1],
            r_ssem.at[1, j],
            r_rsem.at[1, j],
            at_y(j),
        )
        for j in range(1, 4)
    ]
    multiply(x)
    multiply(4 + x)
    p3 = pair_part(3, x)

    e0.wait_recv()
    e4 = early_part(left, 4, 3, 0)
    e1.wait_recv()
    e5 = early_part(4 + right, 5, 1, 1)
    p0.wait_recv()
    pair_sum(0, far)
    l0 = late_part(far, a_at, late_a, 0, 3)
    l1 = late_part(far, b_at, late_b, 1, 1)

    for copy in s1:
        copy.wait_recv()
    r2[...] = r1[pl.ds(pl.multiple_of(y * 8, 8), 8), :] + r_in1[0] + r_in1[1] + r_in1[2]
    s2 = [
        send(
            r2.at[:, pl.ds(pl.multiple_of(((z + j) % 4) * r_cols, LANES), r_cols)],
            r_in2.at[j - 1],
            r_ssem.at[2, j],
            r_rsem.at[2, j],
            at_z(j),
        )
        for j in range(1, 4)
    ]
    p1.wait_recv()
    pair_sum(1, right)
    l2 = late_part(right, a_at, late_a, 2, 1)
    for copy in s2:
        copy.wait_recv()
    r3[...] = r2[:, pl.ds(pl.multiple_of(z * r_cols, LANES), r_cols)] + r_in2[0] + r_in2[1] + r_in2[2]
    s3 = [
        send(
            r3.at[:, pl.ds(pl.multiple_of(((x + j) % 4) * LANES, LANES), LANES)],
            r_in3.at[j - 1],
            r_ssem.at[3, j],
            r_rsem.at[3, j],
            at_x(j),
        )
        for j in range(1, 4)
    ]
    p2.wait_recv()
    pair_sum(2, left)
    l3 = late_part(left, b_at, late_b, 3, 3)

    for copy in (e2, e3, e4, e5):
        copy.wait_recv()

    def fold(r, i):
        terms[x, r, :] += decode_rows(x_in.at[2], i, wide) + decode_rows(x_in.at[4], i, wide)
        terms[4 + x, r, :] += decode_rows(x_in.at[3], i, wide) + decode_rows(x_in.at[5], i, wide)
        encode_rows(terms[(1 - zl) * 4 + x, r, :], last_out, i)

    tiles(0, early, fold)
    last = send(last_out, last_in, z_ssem.at[4], z_rsem.at[4], pair)
    for copy in s3:
        copy.wait_recv()
    piece[...] = r3[:, pl.ds(pl.multiple_of(x * LANES, LANES), LANES)] + r_in3[0] + r_in3[1] + r_in3[2]
    my_row = core * r_half + y * 8
    z_col = z * r_cols
    x_col = z_col + x * LANES
    rgrad[pl.ds(pl.multiple_of(my_row, 8), 8), pl.ds(pl.multiple_of(x_col, LANES), LANES)] = piece[...]

    def give_back(stage, row, height, col, width, at, size):
        part = rgrad.at[pl.ds(pl.multiple_of(row, 8), height), pl.ds(pl.multiple_of(col, LANES), width)]
        return [
            send(part, part, r_ssem.at[stage, j], r_rsem.at[stage, j], at(j)) for j in range(1, size)
        ]

    b0 = give_back(4, my_row, 8, x_col, LANES, at_x, 4)


    l0.wait_recv()
    l4 = late_part(left, a_at, late_a, 4, 3, 0)
    l1.wait_recv()
    l5 = late_part(right, b_at, late_b, 5, 1, 1)
    p3.wait_recv()
    pair_sum(3, x)
    for copy in b0:
        copy.wait_recv()
    b1 = give_back(5, my_row, 8, z_col, r_cols, at_z, 4)

    own = zl * 4 + x

    def count(values, acc):
        values = values * values
        for a in range(2):
            for b in range(wide // LANES):
                acc = acc + values[a * 8 : a * 8 + 8, b * LANES : (b + 1) * LANES]
        return acc

    def close(start, size, acc, sources):
        def step(n, acc):
            i = pl.ds(pl.multiple_of(n * 16, 16), 16)
            r = pl.ds(pl.multiple_of(start + n * 16, 16), 16)
            values = terms[own, r, :]
            for source in sources:
                values = values + decode_rows(source, i, wide)
            grad[r, :] = values
            return count(values, acc)

        return lax.fori_loop(0, size // 16, step, acc, unroll=True)

    squares = jnp.zeros((8, LANES), F32)
    last.wait_recv()
    squares = close(0, early, squares, (last_in,))
    for copy in b1:
        copy.wait_recv()
    b2 = give_back(6, my_row, 8, 0, wide, at_y, 4)
    for copy in (l2, l4):
        copy.wait_recv()
    squares = close(a_at, late_a, squares, (late_in.at[2], late_in.at[4]))
    for copy in (l3, l5):
        copy.wait_recv()
    squares = close(b_at, late_b, squares, (late_in.at[3], late_in.at[5]))

    squares = squares + piece[...] * piece[...]

    def tell(buf, here, at, size, sem):
        buf[here] = squares
        mine = buf.at[here]
        return [send(mine, mine, n_ssem.at[sem + j], n_rsem.at[sem + j], at(j)) for j in range(1, size)]

    def sum_of(buf, size, group):
        for copy in group:
            copy.wait_recv()
        acc = buf[0]
        for k in range(1, size):
            acc = acc + buf[k]
        return acc

    plane_copies = tell(plane_sums, x * 4 + z, at_plane, 16, 0)
    for copy in b2:
        copy.wait_recv()
    b3 = give_back(7, core * r_half, r_half, 0, wide, at_core, 2)
    squares = sum_of(plane_sums, 16, plane_copies)
    side_copies = tell(side_sums, y * 2 + core, at_side, 8, 16)
    squares = sum_of(side_sums, 8, side_copies)
    total[...] = jnp.broadcast_to(jnp.sum(squares), total.shape)
    for copy in b3:
        copy.wait_recv()
    waits = [e0, e1, e2, e3, e4, e5, l0, l1, l2, l3, l4, l5, p0, p1, p2, p3, last, s0, *s1, *s2, *s3]
    for copy in waits + b0 + b1 + b2 + b3 + plane_copies + side_copies:
        copy.wait_send()


def adam_update(gradient, moment_one, moment_two, weights):
    first_new = beta_first * moment_one + (1.0 - beta_first) * gradient
    second_new = beta_second * moment_two + (1.0 - beta_second) * gradient * gradient
    ratio = first_new / correct_first / (jnp.sqrt(second_new / correct_second) + adam_eps)
    weights_new = weights - learn_rate * (ratio + decay_weight * weights)
    return (weights_new, first_new, second_new)


def in_hbm(array):
    return pltpu.with_memory_space_constraint(array, pltpu.HBM)


def each(act, start=1):
    def step(j, carry):
        act(j)
        return carry

    lax.fori_loop(start, GROUPS, step, 0)


def unpack(piece, size, codes):
    return piece[0:size, :].astype(F32) * scale_of(codes.astype(F32))


def close_kernel(
    limit,
    weight,
    new_master,
    landed0,
    landed1,
    total,
    rgrad,
    r_master,
    r_first,
    r_second,
    weight_out,
    master_out,
    first_out,
    second_out,
    r_master_out,
    r_first_out,
    r_second_out,
    values,
    r_values,
    sem,
):
    rows = new_master.shape[0]
    copies = []

    def put(src, dst):
        copy = pltpu.make_async_copy(src, dst, sem.at[len(copies)])
        copy.start()
        copies.append(copy)

    put(weight, weight_out)
    put(new_master, master_out)
    for k, (landed, out) in enumerate(((landed0, first_out), (landed1, second_out))):
        for g in range(GROUPS):
            code = landed0[g, rows + 8 * k : rows + 8 * k + 1, :]
            values[k, :, g * LANES : (g + 1) * LANES] = unpack(landed.at[g], rows, code)
        put(values.at[k], out)
    factor = jnp.minimum(1.0, limit / (jnp.sqrt(total[0:1, 0:1]) + norm_eps))
    new = adam_update(factor * rgrad[...], r_first[...], r_second[...], r_master[...])
    for k, out in enumerate((r_master_out, r_first_out, r_second_out)):
        r_values[k] = new[k]
        put(r_values.at[k], out)
    for copy in copies:
        copy.wait()


def move_kernel(
    limit,
    grad,
    total,
    master,
    first,
    second,
    partner,
    weight,
    new_master,
    landed0,
    landed1,
    lead_out0,
    lead_out1,
    lead_mid0,
    lead_mid1,
    lead_turn0,
    lead_turn1,
    lead_land0,
    lead_land1,
    lead_twin0,
    lead_twin1,
    leaving0,
    leaving1,
    middle0,
    middle1,
    turned0,
    turned1,
    l_ssem,
    l_rsem,
    ssem,
    rsem,
    a_ssem,
    a_rsem,
):
    zl, x, e = (lax.axis_index(a) for a in ALL)
    rows, wide = grad.shape
    half = wide // 2
    lead_out, lead_mid = (lead_out0, lead_out1), (lead_mid0, lead_mid1)
    lead_turn, lead_land, lead_twin = (lead_turn0, lead_turn1), (lead_land0, lead_land1), (lead_twin0, lead_twin1)
    leaving, middle = (leaving0, leaving1), (middle0, middle1)
    turned, landed = (turned0, turned1), (landed0, landed1)
    split = lead_out0.shape[1] - 16
    runs = ((0, split), (split, rows - split))

    def peer(j):
        return {"e": (e + j) % GROUPS}

    def twin_peer(j):
        return {"e": (e + j) % GROUPS, "zl": 1 - zl}

    def at_x(j):
        return {"x": (x + j) % 4}

    barrier = pltpu.get_barrier_semaphore()
    each(lambda j: pl.semaphore_signal(barrier, inc=1, device_id=peer(j), device_id_type=MESH))
    each(lambda j: pl.semaphore_signal(barrier, inc=1, device_id=twin_peer(j), device_id_type=MESH), 0)
    for device in (at_x(1), at_x(3)):
        pl.semaphore_signal(barrier, inc=1, device_id=device, device_id_type=MESH)

    factor = jnp.minimum(1.0, limit / (jnp.sqrt(total[0:1, 0:1]) + norm_eps))

    def columns(g):
        return pl.ds(pl.multiple_of(g * LANES, LANES), LANES)

    def update(g):
        c = columns(g)
        return adam_update(factor * grad[:, c], first[:, c], second[:, c], master[:, c])

    def column_code(values):
        return code_of(jnp.max(jnp.abs(values), axis=0, keepdims=True))

    def pack_lead(g):
        values = update(g)[0]
        code = column_code(values)
        for h, (start, size) in enumerate(runs):
            lead_out[h][g, 0:size, :] = to_codes(values[start : start + size], code)
        lead_out[0][g, split:, :] = jnp.broadcast_to(code, (16, LANES)).astype(I16)

    def remote(src, dst, send_sem, recv_sem, device):
        return pltpu.make_async_remote_copy(
            src_ref=src,
            dst_ref=dst,
            send_sem=send_sem,
            recv_sem=recv_sem,
            device_id=device,
            device_id_type=MESH,
        )

    def lead_go(h, j):
        at = (0, h, j)
        return remote(lead_out[h].at[(e + j) % GROUPS], lead_mid[h].at[j], l_ssem.at[at], l_rsem.at[at], peer(j))

    def lead_come(h, j):
        at = (1, h, j)
        src = lead_turn[h].at[(e + j) % GROUPS]
        return remote(src, lead_land[h].at[e], l_ssem.at[at], l_rsem.at[at], peer(j))

    def lead_cross(h, j):
        at = (2, h, j)
        src = lead_turn[h].at[(e + j) % GROUPS]
        return remote(src, lead_twin[h].at[e], l_ssem.at[at], l_rsem.at[at], twin_peer(j))

    def go(k, j):
        at = (0, k, j)
        return remote(leaving[k].at[(e + j) % GROUPS], middle[k].at[j], ssem.at[at], rsem.at[at], peer(j))

    def come(k, j):
        at = (1, k, j)
        return remote(turned[k].at[(e + j) % GROUPS], landed[k].at[e], ssem.at[at], rsem.at[at], peer(j))

    def permute(arrived, to):
        def step(p, carry):
            to[p] = arrived[(e - partner[p] + GROUPS) % GROUPS]
            return carry

        lax.fori_loop(0, GROUPS, step, 0)

    pack_lead(e)
    pl.semaphore_wait(barrier, 2 * GROUPS + 1)

    def first_leg(j):
        pack_lead((e + j) % GROUPS)
        lead_go(0, j).start()

    each(first_leg)
    each(lambda j: lead_go(1, j).start())
    for h in range(2):
        lead_mid[h][0] = lead_out[h][e]

    for h in range(2):
        each(lambda j, h=h: lead_go(h, j).wait_recv())
        permute(lead_mid[h], lead_turn[h])
        each(lambda j, h=h: lead_come(h, j).start())
        lead_land[h][e] = lead_turn[h][e]
    for h in range(2):
        each(lambda j, h=h: lead_cross(h, j).start(), 0)

    def moments(g):
        _, first_new, second_new = update(g)
        code = column_code(first_new), column_code(second_new)
        leaving0[g, 0:rows, :] = to_codes(first_new, code[0])
        leaving1[g] = to_codes(second_new, code[1])
        both = [jnp.broadcast_to(c, (8, LANES)) for c in code]
        leaving0[g, rows:, :] = jnp.concatenate(both, axis=0).astype(I16)

    each(moments, 0)

    own, twin = zl * 4 + x, (1 - zl) * 4 + x
    left, right = (x + 3) % 4, (x + 1) % 4

    def weight_rows(block, h):
        return pl.ds(pl.multiple_of(block * rows + runs[h][0], 16), runs[h][1])

    def gather(n, h, block, col, width, device):
        part = weight.at[weight_rows(block, h), pl.ds(col, width)]
        return send(part, part, a_ssem.at[n, h], a_rsem.at[n, h], device)

    def settle(h, g):
        values = unpack(lead_land[h].at[g], runs[h][1], lead_land0[g, split : split + 1, :])
        new_master[pl.ds(*runs[h]), columns(g)] = values
        weight[weight_rows(own, h), columns(g)] = values.astype(jnp.bfloat16)

    def settle_twin(h, g):
        values = unpack(lead_twin[h].at[g], runs[h][1], lead_twin0[g, split : split + 1, :])
        weight[weight_rows(twin, h), columns(g)] = values.astype(jnp.bfloat16)

    to_right, to_left = [], []
    for h in range(2):
        settle(h, e)

        def settle_next(j, h=h):
            lead_come(h, j).wait_recv()
            settle(h, (e - j + GROUPS) % GROUPS)

        each(settle_next)
        to_right.append(gather(0, h, own, 0, wide, at_x(1)))
        to_left.append(gather(1, h, own, 0, wide, at_x(3)))

    each(lambda j: go(0, j).start())
    each(lambda j: go(1, j).start())

    twin_right, twin_left = [], []
    for h in range(2):

        def settle_cross(j, h=h):
            lead_cross(h, j).wait_recv()
            settle_twin(h, (e - j + GROUPS) % GROUPS)

        each(settle_cross, 0)
        twin_right.append(gather(2, h, twin, 0, wide, at_x(1)))
        twin_left.append(gather(3, h, twin, 0, wide, at_x(3)))

    onward = []

    def pass_on(n, h, z_at, from_left, from_right):
        from_left.wait_recv()
        onward.append(gather(n, h, z_at * 4 + left, 0, half, at_x(1)))
        from_right.wait_recv()
        onward.append(gather(n + 1, h, z_at * 4 + right, half, half, at_x(3)))

    def turn(k):
        each(lambda j: go(k, j).wait_recv())
        middle[k][0] = leaving[k][e]
        permute(middle[k], turned[k])
        each(lambda j: come(k, j).start())
        landed[k][e] = turned[k][e]

    pass_on(4, 0, zl, to_right[0], to_left[0])
    pass_on(4, 1, zl, to_right[1], to_left[1])
    turn(0)
    pass_on(6, 0, 1 - zl, twin_right[0], twin_left[0])
    turn(1)
    pass_on(6, 1, 1 - zl, twin_right[1], twin_left[1])

    for k in range(2):
        each(lambda j, k=k: come(k, j).wait_recv())
    for copy in onward:
        copy.wait_recv()
    for k in range(2):
        each(lambda j, k=k: lead_go(k, j).wait_send())
        each(lambda j, k=k: lead_come(k, j).wait_send())
        each(lambda j, k=k: lead_cross(k, j).wait_send(), 0)
        each(lambda j, k=k: go(k, j).wait_send())
        each(lambda j, k=k: come(k, j).wait_send())
    for copy in to_right + to_left + twin_right + twin_left + onward:
        copy.wait_send()


def on_device(
    hidden,
    upstream,
    token_counts,
    master,
    first_moment,
    second_moment,
    router_input,
    router_cot,
    router_master,
    router_first,
    router_second,
    partner,
):
    depth, units = hidden.shape[1:]
    wide = upstream.shape[2]
    rows = units // 8
    n_router = router_cot.shape[0]
    vmem = pl.BlockSpec(memory_space=pltpu.VMEM)
    smem = pl.BlockSpec(memory_space=pltpu.SMEM)
    hbm = pl.BlockSpec(memory_space=pltpu.HBM)
    dma = pltpu.SemaphoreType.DMA
    coded = wide + LANES
    r_half, r_cols = n_router // 2, wide // 4
    late = rows * 5 // 11 // 16 * 16
    early = rows - late
    late_a = (late // 16 + 1) // 2 * 16
    gradient, router_grad, total = pl.pallas_call(
        reduce_kernel,
        out_shape=(
            jax.ShapeDtypeStruct((rows, wide), F32),
            jax.ShapeDtypeStruct((n_router, wide), F32),
            jax.ShapeDtypeStruct((8, LANES), F32),
        ),
        in_specs=[hbm, hbm, smem, hbm, hbm],
        out_specs=(vmem, vmem, vmem),
        scratch_shapes=[
            pltpu.VMEM((depth, units), jnp.bfloat16),
            pltpu.VMEM((depth, wide), jnp.bfloat16),
            pltpu.VMEM(router_cot.shape, jnp.bfloat16),
            pltpu.VMEM(router_input.shape, jnp.bfloat16),
            pltpu.VMEM((units, depth), jnp.bfloat16),
            pltpu.VMEM((8, rows, wide), F32),
            *[pltpu.VMEM((6, early, coded), I16)] * 2,
            *[pltpu.VMEM((6, late_a, coded), I16)] * 2,
            *[pltpu.VMEM((4, late, coded), I16)] * 2,
            *[pltpu.VMEM((early, coded), I16)] * 2,
            pltpu.VMEM((n_router, wide), F32),
            pltpu.VMEM((r_half, wide), F32),
            pltpu.VMEM((r_half, wide), F32),
            pltpu.VMEM((3, 8, wide), F32),
            pltpu.VMEM((8, wide), F32),
            pltpu.VMEM((3, 8, r_cols), F32),
            pltpu.VMEM((8, r_cols), F32),
            pltpu.VMEM((3, 8, LANES), F32),
            pltpu.VMEM((8, LANES), F32),
            pltpu.VMEM((16, 8, LANES), F32),
            pltpu.VMEM((8, 8, LANES), F32),
            dma((4,)),
            dma((12,)),
            dma((12,)),
            dma((5,)),
            dma((5,)),
            dma((8, 4)),
            dma((8, 4)),
            dma((24,)),
            dma((24,)),
        ],
        compiler_params=pltpu.CompilerParams(
            collective_id=0, has_side_effects=True, vmem_limit_bytes=40 * 1024 * 1024
        ),
        name="reduce",
    )(in_hbm(hidden[0]), in_hbm(upstream[0]), token_counts, in_hbm(router_cot), in_hbm(router_input))

    clip_limit = 2.0 * math.sqrt(float(GROUPS * units * wide + n_router * wide))
    split = (rows // 16 + 1) // 2 * 16
    state = jax.ShapeDtypeStruct((rows, wide), F32)
    codes = [jax.ShapeDtypeStruct((GROUPS, n, LANES), I16) for n in (rows + 16, rows)]
    weights = jax.ShapeDtypeStruct((units, wide), jnp.bfloat16)
    weight, new_master, *landed = pl.pallas_call(
        functools.partial(move_kernel, clip_limit),
        out_shape=(weights, state, *codes),
        in_specs=[vmem, vmem, vmem, vmem, vmem, smem],
        out_specs=(vmem, vmem, vmem, vmem),
        scratch_shapes=[
            *[pltpu.VMEM((GROUPS, n, LANES), I16) for n in (split + 16, rows - split)] * 5,
            *[pltpu.VMEM((GROUPS, n, LANES), I16) for n in (rows + 16, rows)] * 3,
            dma((3, 2, GROUPS)),
            dma((3, 2, GROUPS)),
            dma((2, 2, GROUPS)),
            dma((2, 2, GROUPS)),
            dma((8, 2)),
            dma((8, 2)),
        ],
        compiler_params=pltpu.CompilerParams(
            collective_id=1, has_side_effects=True, vmem_limit_bytes=27 * 1024 * 1024
        ),
        name="move",
    )(gradient, total, master[0], first_moment[0], second_moment[0], partner)

    router = jax.ShapeDtypeStruct(router_master.shape, F32)
    weight, new_master, new_first, new_second, *router_outs = pl.pallas_call(
        functools.partial(close_kernel, clip_limit),
        out_shape=(weights, state, state, state, router, router, router),
        in_specs=[vmem] * 9,
        out_specs=[hbm] * 7,
        scratch_shapes=[
            pltpu.VMEM((2, rows, wide), F32),
            pltpu.VMEM((3, *router_master.shape), F32),
            dma((7,)),
        ],
        compiler_params=pltpu.CompilerParams(vmem_limit_bytes=20 * 1024 * 1024),
        name="close",
    )(weight, new_master, *landed, total, router_grad, router_master, router_first, router_second)
    return (weight[None], new_master[None], new_first[None], new_second[None], *router_outs)


def solution(mesh):
    split = Mesh(mesh.devices.reshape(2, 4, mesh.shape["expert"]), ALL)
    return jax.shard_map(
        on_device,
        mesh=split,
        in_specs=(
            P("e", DP, None),
            P("e", DP, None),
            P("e", DP),
            P("e", DP, None),
            P("e", DP, None),
            P("e", DP, None),
            P(ALL, None),
            P(None, ALL),
            P(),
            P(),
            P(),
            P(),
        ),
        out_specs=(
            P("e", None, None),
            P("e", DP, None),
            P("e", DP, None),
            P("e", DP, None),
            P(),
            P(),
            P(),
        ),
        check_vma=False,
    )
```

```python
import functools
import math

import jax
import jax.numpy as jnp
from jax import lax
from jax.experimental import pallas as pl
from jax.experimental.pallas import tpu as pltpu
from jax.sharding import Mesh
from jax.sharding import PartitionSpec as P

MESH = pl.DeviceIdType.MESH
DP = ("zl", "x")
ALL = ("zl", "x", "e")
F32 = jnp.float32
I16 = jnp.int16

beta_first = 0.9
beta_second = 0.95
learn_rate = 0.001
decay_weight = 0.1
adam_eps = 1e-08
norm_eps = 1e-06
correct_first = 1.0 - 0.9**10
correct_second = 1.0 - 0.95**10

GROUPS = 16
LANES = 128
TOP = 15.0
SMALL = 2.0**-100
MOVE_SCRATCH = 22


def code_of(peak):
    return jnp.ceil(16.0 * jnp.log2(jnp.maximum(peak, SMALL)))


def to_codes(values, code):
    scaled = jnp.round(values * jnp.exp2(TOP - code * (1.0 / 16.0)))
    return jnp.clip(scaled, -32767.0, 32767.0).astype(I16)


def scale_of(code):
    return jnp.exp2(code * (1.0 / 16.0) - TOP)


def encode_rows(values, dst, rows):
    width = values.shape[1]
    code = code_of(jnp.max(jnp.abs(values), axis=1, keepdims=True))
    dst[rows, :width] = to_codes(values, code)
    dst[rows, width:] = jnp.broadcast_to(code, (values.shape[0], LANES)).astype(I16)


def decode_rows(src, rows, width):
    code = src[rows, width : width + LANES].astype(F32)[:, :1]
    return src[rows, :width].astype(F32) * scale_of(code)


def send(src, dst, send_sem, recv_sem, device):
    copy = pltpu.make_async_remote_copy(
        src_ref=src, dst_ref=dst, send_sem=send_sem, recv_sem=recv_sem, device_id=device, device_id_type=MESH
    )
    copy.start()
    return copy


def each(act, start=1):
    def step(j, carry):
        act(j)
        return carry

    lax.fori_loop(start, GROUPS, step, 0)


def reduce_kernel(
    states,
    hid_hbm,
    up_hbm,
    counts,
    cot_hbm,
    rin_hbm,
    rgrad,
    total,
    hid,
    up,
    cot,
    rin,
    hid_t,
    terms,
    x_out,
    x_in,
    late_out,
    late_in,
    z_out,
    z_in,
    last_out,
    last_in,
    rp,
    r_in0,
    r1,
    r_in1,
    r2,
    r_in2,
    r3,
    r_in3,
    piece,
    plane_sums,
    side_sums,
    load_sem,
    x_ssem,
    x_rsem,
    z_ssem,
    z_rsem,
    r_ssem,
    r_rsem,
    n_ssem,
    n_rsem,
):
    zl, x, e = (lax.axis_index(a) for a in ALL)
    y, zh, core = e // 4, (e // 2) % 2, e % 2
    z = zh * 2 + zl
    depth, units = hid.shape
    wide = up.shape[1]
    rows = units // 8
    early = x_out.shape[1]
    late = rows - early
    late_a = late_out.shape[1]
    late_b = late - late_a

    def at_x(j):
        return {"x": (x + j) % 4}

    def at_z(j):
        there = (z + j) % 4
        return {"zl": there % 2, "e": y * 4 + (there // 2) * 2 + core}

    def at_y(j):
        return {"e": ((y + j) % 4) * 4 + zh * 2 + core}

    def at_core(j):
        return {"e": e + 1 - 2 * core}

    pair = {"zl": 1 - zl}

    def at_plane(j):
        there = (z + j % 4) % 4
        return {"x": (x + j // 4) % 4, "zl": there % 2, "e": y * 4 + (there // 2) * 2 + core}

    def at_side(j):
        return {"e": ((y + j // 2) % 4) * 4 + zh * 2 + (core + j) % 2}

    loads = [
        pltpu.make_async_copy(src, dst, load_sem.at[n])
        for n, (src, dst) in enumerate(((hid_hbm, hid), (up_hbm, up), (cot_hbm, cot), (rin_hbm, rin)))
    ]
    for copy in loads:
        copy.start()
    barrier = pltpu.get_barrier_semaphore()
    for j in range(1, 16):
        pl.semaphore_signal(barrier, inc=1, device_id=at_plane(j), device_id_type=MESH)

    def greet(device):
        pl.semaphore_signal(barrier, inc=1, device_id=device, device_id_type=MESH)

    each(lambda j: greet({"e": (e + j) % GROUPS}))
    each(lambda j: greet({"e": (e + j) % GROUPS, "zl": 1 - zl}), 0)

    live = counts[0, 0]
    keep = (lax.broadcasted_iota(jnp.int32, (depth, LANES), 0) < live).astype(F32).astype(jnp.bfloat16)
    loads[0].wait()

    @pl.loop(0, units // LANES)
    def _(t):
        cols = pl.ds(pl.multiple_of(t * LANES, LANES), LANES)
        hid_t[cols, :] = (hid[:, cols] * keep).T

    def multiply(block):
        at = pl.multiple_of(block * rows, 16)

        @pl.loop(0, wide // 512)
        def _(n):
            cols = pl.ds(pl.multiple_of(n * 512, 512), 512)
            terms[block, :, cols] = jnp.dot(hid_t[pl.ds(at, rows), :], up[:, cols], preferred_element_type=F32)

    def tiles(start, size, act):
        @pl.loop(0, size // 16, unroll=True)
        def _(i):
            act(
                pl.ds(pl.multiple_of(start + i * 16, 16), 16),
                pl.ds(pl.multiple_of(i * 16, 16), 16),
            )

    def x_made(slot, device):
        return pltpu.make_async_remote_copy(
            src_ref=x_out.at[slot],
            dst_ref=x_in.at[slot],
            send_sem=x_ssem.at[slot],
            recv_sem=x_rsem.at[slot],
            device_id=device,
            device_id_type=MESH,
        )

    def x_copy(slot, device):
        copy = x_made(slot, device)
        copy.start()
        return copy

    def late_copy(slot, size, device):
        r = pl.ds(0, size)
        return send(
            late_out.at[slot, r], late_in.at[slot, r], x_ssem.at[6 + slot], x_rsem.at[6 + slot], device
        )

    def early_part(block, slot, step, incoming=None):
        def act(r, i):
            values = terms[block, r, :]
            if incoming is not None:
                values = values + decode_rows(x_in.at[incoming], i, wide)
            encode_rows(values, x_out.at[slot], i)

        tiles(0, early, act)
        return x_copy(slot, at_x(step))

    def pair_part(n, there):
        def act(r, i):
            encode_rows(terms[(1 - zl) * 4 + there, r, :], z_out.at[n], i)

        tiles(early, late, act)
        return send(z_out.at[n], z_in.at[n], z_ssem.at[n], z_rsem.at[n], pair)

    def pair_sum(n, there):
        block = zl * 4 + there

        def act(r, i):
            terms[block, r, :] += decode_rows(z_in.at[n], i, wide)

        tiles(early, late, act)

    def late_part(there, start, size, slot, step, incoming=None):
        block = zl * 4 + there

        def act(r, i):
            values = terms[block, r, :]
            if incoming is not None:
                values = values + decode_rows(late_in.at[incoming], i, wide)
            encode_rows(values, late_out.at[slot], i)

        tiles(start, size, act)
        return late_copy(slot, size, at_x(step))

    far, right, left = (x + 2) % 4, (x + 1) % 4, (x + 3) % 4
    a_at, b_at = early, early + late_a

    loads[1].wait()
    multiply((1 - zl) * 4 + far)
    pl.semaphore_wait(barrier, 15 + 15 + 16)
    p0 = pair_part(0, far)
    early_part((1 - zl) * 4 + far, 1 - zl, 1 + 2 * zl)
    multiply(zl * 4 + far)
    early_part(zl * 4 + far, zl, 3 - 2 * zl)
    e0, e1 = x_made(0, at_x(3)), x_made(1, at_x(1))
    multiply(right)
    e2 = early_part(right, 2, 1)
    multiply(4 + left)
    e3 = early_part(4 + left, 3, 3)
    multiply(4 + right)
    p1 = pair_part(1, right)

    loads[2].wait()
    loads[3].wait()
    rp[...] = jnp.dot(cot[...], rin[...], preferred_element_type=F32)
    n_router = rp.shape[0]
    r_half, r_cols = n_router // 2, wide // 4
    s0 = send(
        rp.at[pl.ds(pl.multiple_of((1 - core) * r_half, 8), r_half)],
        r_in0,
        r_ssem.at[0, 1],
        r_rsem.at[0, 1],
        at_core(1),
    )
    multiply(left)
    p2 = pair_part(2, left)
    s0.wait_recv()
    r1[...] = rp[pl.ds(pl.multiple_of(core * r_half, 8), r_half), :] + r_in0[...]
    s1 = [
        send(
            r1.at[pl.ds(pl.multiple_of(((y + j) % 4) * 8, 8), 8)],
            r_in1.at[j - 1],
            r_ssem.at[1, j],
            r_rsem.at[1, j],
            at_y(j),
        )
        for j in range(1, 4)
    ]
    multiply(x)
    multiply(4 + x)
    p3 = pair_part(3, x)

    e0.wait_recv()
    e4 = early_part(left, 4, 3, 0)
    e1.wait_recv()
    e5 = early_part(4 + right, 5, 1, 1)
    p0.wait_recv()
    pair_sum(0, far)
    l0 = late_part(far, a_at, late_a, 0, 3)
    l1 = late_part(far, b_at, late_b, 1, 1)

    held = [terms.at[block] for block in (far, 4 + far, (1 - zl) * 4 + right)]
    state_loads = [pltpu.make_async_copy(src, dst, states[3].at[k]) for k, (src, dst) in enumerate(zip(states, held))]
    for copy in state_loads:
        copy.start()

    for copy in s1:
        copy.wait_recv()
    r2[...] = r1[pl.ds(pl.multiple_of(y * 8, 8), 8), :] + r_in1[0] + r_in1[1] + r_in1[2]
    s2 = [
        send(
            r2.at[:, pl.ds(pl.multiple_of(((z + j) % 4) * r_cols, LANES), r_cols)],
            r_in2.at[j - 1],
            r_ssem.at[2, j],
            r_rsem.at[2, j],
            at_z(j),
        )
        for j in range(1, 4)
    ]
    p1.wait_recv()
    pair_sum(1, right)
    l2 = late_part(right, a_at, late_a, 2, 1)
    for copy in s2:
        copy.wait_recv()
    r3[...] = r2[:, pl.ds(pl.multiple_of(z * r_cols, LANES), r_cols)] + r_in2[0] + r_in2[1] + r_in2[2]
    s3 = [
        send(
            r3.at[:, pl.ds(pl.multiple_of(((x + j) % 4) * LANES, LANES), LANES)],
            r_in3.at[j - 1],
            r_ssem.at[3, j],
            r_rsem.at[3, j],
            at_x(j),
        )
        for j in range(1, 4)
    ]
    p2.wait_recv()
    pair_sum(2, left)
    l3 = late_part(left, b_at, late_b, 3, 3)

    for copy in (e2, e3, e4, e5):
        copy.wait_recv()

    def fold(r, i):
        terms[x, r, :] += decode_rows(x_in.at[2], i, wide) + decode_rows(x_in.at[4], i, wide)
        terms[4 + x, r, :] += decode_rows(x_in.at[3], i, wide) + decode_rows(x_in.at[5], i, wide)
        encode_rows(terms[(1 - zl) * 4 + x, r, :], last_out, i)

    tiles(0, early, fold)
    last = send(last_out, last_in, z_ssem.at[4], z_rsem.at[4], pair)
    for copy in s3:
        copy.wait_recv()
    piece[...] = r3[:, pl.ds(pl.multiple_of(x * LANES, LANES), LANES)] + r_in3[0] + r_in3[1] + r_in3[2]
    my_row = core * r_half + y * 8
    z_col = z * r_cols
    x_col = z_col + x * LANES
    rgrad[pl.ds(pl.multiple_of(my_row, 8), 8), pl.ds(pl.multiple_of(x_col, LANES), LANES)] = piece[...]

    def give_back(stage, row, height, col, width, at, size):
        part = rgrad.at[pl.ds(pl.multiple_of(row, 8), height), pl.ds(pl.multiple_of(col, LANES), width)]
        return [
            send(part, part, r_ssem.at[stage, j], r_rsem.at[stage, j], at(j)) for j in range(1, size)
        ]

    b0 = give_back(4, my_row, 8, x_col, LANES, at_x, 4)


    l0.wait_recv()
    l4 = late_part(left, a_at, late_a, 4, 3, 0)
    l1.wait_recv()
    l5 = late_part(right, b_at, late_b, 5, 1, 1)
    p3.wait_recv()
    pair_sum(3, x)
    for copy in b0:
        copy.wait_recv()
    b1 = give_back(5, my_row, 8, z_col, r_cols, at_z, 4)

    own = zl * 4 + x

    def count(values, acc):
        values = values * values
        for a in range(2):
            for b in range(wide // LANES):
                acc = acc + values[a * 8 : a * 8 + 8, b * LANES : (b + 1) * LANES]
        return acc

    def close(start, size, acc, sources):
        def step(n, acc):
            i = pl.ds(pl.multiple_of(n * 16, 16), 16)
            r = pl.ds(pl.multiple_of(start + n * 16, 16), 16)
            values = terms[own, r, :]
            for source in sources:
                values = values + decode_rows(source, i, wide)
            terms[own, r, :] = values
            return count(values, acc)

        return lax.fori_loop(0, size // 16, step, acc, unroll=True)

    squares = jnp.zeros((8, LANES), F32)
    last.wait_recv()
    squares = close(0, early, squares, (last_in,))
    for copy in b1:
        copy.wait_recv()
    b2 = give_back(6, my_row, 8, 0, wide, at_y, 4)
    for copy in (l2, l4):
        copy.wait_recv()
    squares = close(a_at, late_a, squares, (late_in.at[2], late_in.at[4]))
    for copy in (l3, l5):
        copy.wait_recv()
    squares = close(b_at, late_b, squares, (late_in.at[3], late_in.at[5]))

    squares = squares + piece[...] * piece[...]

    def tell(buf, here, at, size, sem):
        buf[here] = squares
        mine = buf.at[here]
        return [send(mine, mine, n_ssem.at[sem + j], n_rsem.at[sem + j], at(j)) for j in range(1, size)]

    def sum_of(buf, size, group):
        for copy in group:
            copy.wait_recv()
        acc = buf[0]
        for k in range(1, size):
            acc = acc + buf[k]
        return acc

    plane_copies = tell(plane_sums, x * 4 + z, at_plane, 16, 0)
    for copy in b2:
        copy.wait_recv()
    b3 = give_back(7, core * r_half, r_half, 0, wide, at_core, 2)
    squares = sum_of(plane_sums, 16, plane_copies)
    side_copies = tell(side_sums, y * 2 + core, at_side, 8, 16)
    squares = sum_of(side_sums, 8, side_copies)
    total[...] = jnp.broadcast_to(jnp.sum(squares), total.shape)
    for copy in b3:
        copy.wait_recv()
    waits = [e0, e1, e2, e3, e4, e5, l0, l1, l2, l3, l4, l5, p0, p1, p2, p3, last, s0, *s1, *s2, *s3]
    for copy in waits + b0 + b1 + b2 + b3 + plane_copies + side_copies:
        copy.wait_send()
    return state_loads, terms.at[own], held


def step_kernel(limit, *refs):
    (hid, up, counts, cot, rin, master_hbm, first_hbm, second_hbm, partner), refs = refs[:9], refs[9:]
    (rgrad, total, weight, new_master, landed0, landed1), refs = refs[:6], refs[6:]
    state_sem, refs = refs[0], refs[1:]
    n = len(refs) - MOVE_SCRATCH
    states = (master_hbm, first_hbm, second_hbm, state_sem)
    loads, grad, held = reduce_kernel(states, hid, up, counts, cot, rin, rgrad, total, *refs[:n])
    for copy in loads:
        copy.wait()
    outs = (weight, new_master, landed0, landed1)
    move_kernel(limit, grad, total, *held, partner, *outs, *refs[n:])


def adam_update(gradient, moment_one, moment_two, weights):
    first_new = beta_first * moment_one + (1.0 - beta_first) * gradient
    second_new = beta_second * moment_two + (1.0 - beta_second) * gradient * gradient
    ratio = first_new / correct_first / (jnp.sqrt(second_new / correct_second) + adam_eps)
    weights_new = weights - learn_rate * (ratio + decay_weight * weights)
    return (weights_new, first_new, second_new)


def in_hbm(array):
    return pltpu.with_memory_space_constraint(array, pltpu.HBM)


def unpack(piece, size, codes):
    return piece[0:size, :].astype(F32) * scale_of(codes.astype(F32))


def close_kernel(
    limit,
    weight,
    new_master,
    landed0,
    landed1,
    total,
    rgrad,
    r_master,
    r_first,
    r_second,
    weight_out,
    master_out,
    first_out,
    second_out,
    r_master_out,
    r_first_out,
    r_second_out,
    values,
    r_values,
    sem,
):
    rows = new_master.shape[0]
    copies = []

    def put(src, dst):
        copy = pltpu.make_async_copy(src, dst, sem.at[len(copies)])
        copy.start()
        copies.append(copy)

    put(weight, weight_out)
    put(new_master, master_out)
    for k, (landed, out) in enumerate(((landed0, first_out), (landed1, second_out))):
        for g in range(GROUPS):
            code = landed0[g, rows + 8 * k : rows + 8 * k + 1, :]
            values[k, :, g * LANES : (g + 1) * LANES] = unpack(landed.at[g], rows, code)
        put(values.at[k], out)
    factor = jnp.minimum(1.0, limit / (jnp.sqrt(total[0:1, 0:1]) + norm_eps))
    new = adam_update(factor * rgrad[...], r_first[...], r_second[...], r_master[...])
    for k, out in enumerate((r_master_out, r_first_out, r_second_out)):
        r_values[k] = new[k]
        put(r_values.at[k], out)
    for copy in copies:
        copy.wait()


def move_kernel(
    limit,
    grad,
    total,
    master,
    first,
    second,
    partner,
    weight,
    new_master,
    landed0,
    landed1,
    lead_out0,
    lead_out1,
    lead_mid0,
    lead_mid1,
    lead_turn0,
    lead_turn1,
    lead_land0,
    lead_land1,
    lead_twin0,
    lead_twin1,
    leaving0,
    leaving1,
    middle0,
    middle1,
    turned0,
    turned1,
    l_ssem,
    l_rsem,
    ssem,
    rsem,
    a_ssem,
    a_rsem,
):
    zl, x, e = (lax.axis_index(a) for a in ALL)
    rows, wide = grad.shape
    half = wide // 2
    lead_out, lead_mid = (lead_out0, lead_out1), (lead_mid0, lead_mid1)
    lead_turn, lead_land, lead_twin = (lead_turn0, lead_turn1), (lead_land0, lead_land1), (lead_twin0, lead_twin1)
    leaving, middle = (leaving0, leaving1), (middle0, middle1)
    turned, landed = (turned0, turned1), (landed0, landed1)
    split = lead_out0.shape[1] - 16
    runs = ((0, split), (split, rows - split))

    def peer(j):
        return {"e": (e + j) % GROUPS}

    def twin_peer(j):
        return {"e": (e + j) % GROUPS, "zl": 1 - zl}

    def at_x(j):
        return {"x": (x + j) % 4}

    factor = jnp.minimum(1.0, limit / (jnp.sqrt(total[0:1, 0:1]) + norm_eps))

    def columns(g):
        return pl.ds(pl.multiple_of(g * LANES, LANES), LANES)

    def update(g):
        c = columns(g)
        return adam_update(factor * grad[:, c], first[:, c], second[:, c], master[:, c])

    def column_code(values):
        return code_of(jnp.max(jnp.abs(values), axis=0, keepdims=True))

    def pack_lead(g):
        values = update(g)[0]
        code = column_code(values)
        for h, (start, size) in enumerate(runs):
            lead_out[h][g, 0:size, :] = to_codes(values[start : start + size], code)
        lead_out[0][g, split:, :] = jnp.broadcast_to(code, (16, LANES)).astype(I16)

    def remote(src, dst, send_sem, recv_sem, device):
        return pltpu.make_async_remote_copy(
            src_ref=src,
            dst_ref=dst,
            send_sem=send_sem,
            recv_sem=recv_sem,
            device_id=device,
            device_id_type=MESH,
        )

    def lead_go(h, j):
        at = (0, h, j)
        return remote(lead_out[h].at[(e + j) % GROUPS], lead_mid[h].at[j], l_ssem.at[at], l_rsem.at[at], peer(j))

    def lead_come(h, j):
        at = (1, h, j)
        src = lead_turn[h].at[(e + j) % GROUPS]
        return remote(src, lead_land[h].at[e], l_ssem.at[at], l_rsem.at[at], peer(j))

    def lead_cross(h, j):
        at = (2, h, j)
        src = lead_turn[h].at[(e + j) % GROUPS]
        return remote(src, lead_twin[h].at[e], l_ssem.at[at], l_rsem.at[at], twin_peer(j))

    def go(k, j):
        at = (0, k, j)
        return remote(leaving[k].at[(e + j) % GROUPS], middle[k].at[j], ssem.at[at], rsem.at[at], peer(j))

    def come(k, j):
        at = (1, k, j)
        return remote(turned[k].at[(e + j) % GROUPS], landed[k].at[e], ssem.at[at], rsem.at[at], peer(j))

    def permute(arrived, to):
        def step(p, carry):
            to[p] = arrived[(e - partner[p] + GROUPS) % GROUPS]
            return carry

        lax.fori_loop(0, GROUPS, step, 0)

    pack_lead(e)

    def first_leg(j):
        pack_lead((e + j) % GROUPS)
        lead_go(0, j).start()

    each(first_leg)
    each(lambda j: lead_go(1, j).start())
    for h in range(2):
        lead_mid[h][0] = lead_out[h][e]

    for h in range(2):
        each(lambda j, h=h: lead_go(h, j).wait_recv())
        permute(lead_mid[h], lead_turn[h])
        each(lambda j, h=h: lead_come(h, j).start())
        lead_land[h][e] = lead_turn[h][e]
    for h in range(2):
        each(lambda j, h=h: lead_cross(h, j).start(), 0)

    def moments(g):
        _, first_new, second_new = update(g)
        code = column_code(first_new), column_code(second_new)
        leaving0[g, 0:rows, :] = to_codes(first_new, code[0])
        leaving1[g] = to_codes(second_new, code[1])
        both = [jnp.broadcast_to(c, (8, LANES)) for c in code]
        leaving0[g, rows:, :] = jnp.concatenate(both, axis=0).astype(I16)

    each(moments, 0)

    own, twin = zl * 4 + x, (1 - zl) * 4 + x
    left, right = (x + 3) % 4, (x + 1) % 4

    def weight_rows(block, h):
        return pl.ds(pl.multiple_of(block * rows + runs[h][0], 16), runs[h][1])

    def gather(n, h, block, col, width, device):
        part = weight.at[weight_rows(block, h), pl.ds(col, width)]
        return send(part, part, a_ssem.at[n, h], a_rsem.at[n, h], device)

    def settle(h, g):
        values = unpack(lead_land[h].at[g], runs[h][1], lead_land0[g, split : split + 1, :])
        new_master[pl.ds(*runs[h]), columns(g)] = values
        weight[weight_rows(own, h), columns(g)] = values.astype(jnp.bfloat16)

    def settle_twin(h, g):
        values = unpack(lead_twin[h].at[g], runs[h][1], lead_twin0[g, split : split + 1, :])
        weight[weight_rows(twin, h), columns(g)] = values.astype(jnp.bfloat16)

    to_right, to_left = [], []
    for h in range(2):
        settle(h, e)

        def settle_next(j, h=h):
            lead_come(h, j).wait_recv()
            settle(h, (e - j + GROUPS) % GROUPS)

        each(settle_next)
        to_right.append(gather(0, h, own, 0, wide, at_x(1)))
        to_left.append(gather(1, h, own, 0, wide, at_x(3)))

    each(lambda j: go(0, j).start())
    each(lambda j: go(1, j).start())

    twin_right, twin_left = [], []
    for h in range(2):

        def settle_cross(j, h=h):
            lead_cross(h, j).wait_recv()
            settle_twin(h, (e - j + GROUPS) % GROUPS)

        each(settle_cross, 0)
        twin_right.append(gather(2, h, twin, 0, wide, at_x(1)))
        twin_left.append(gather(3, h, twin, 0, wide, at_x(3)))

    onward = []

    def pass_on(n, h, z_at, from_left, from_right):
        from_left.wait_recv()
        onward.append(gather(n, h, z_at * 4 + left, 0, half, at_x(1)))
        from_right.wait_recv()
        onward.append(gather(n + 1, h, z_at * 4 + right, half, half, at_x(3)))

    def turn(k):
        each(lambda j: go(k, j).wait_recv())
        middle[k][0] = leaving[k][e]
        permute(middle[k], turned[k])
        each(lambda j: come(k, j).start())
        landed[k][e] = turned[k][e]

    pass_on(4, 0, zl, to_right[0], to_left[0])
    pass_on(4, 1, zl, to_right[1], to_left[1])
    turn(0)
    pass_on(6, 0, 1 - zl, twin_right[0], twin_left[0])
    turn(1)
    pass_on(6, 1, 1 - zl, twin_right[1], twin_left[1])

    for k in range(2):
        each(lambda j, k=k: come(k, j).wait_recv())
    for copy in onward:
        copy.wait_recv()
    for k in range(2):
        each(lambda j, k=k: lead_go(k, j).wait_send())
        each(lambda j, k=k: lead_come(k, j).wait_send())
        each(lambda j, k=k: lead_cross(k, j).wait_send(), 0)
        each(lambda j, k=k: go(k, j).wait_send())
        each(lambda j, k=k: come(k, j).wait_send())
    for copy in to_right + to_left + twin_right + twin_left + onward:
        copy.wait_send()


def on_device(
    hidden,
    upstream,
    token_counts,
    master,
    first_moment,
    second_moment,
    router_input,
    router_cot,
    router_master,
    router_first,
    router_second,
    partner,
):
    depth, units = hidden.shape[1:]
    wide = upstream.shape[2]
    rows = units // 8
    n_router = router_cot.shape[0]
    vmem = pl.BlockSpec(memory_space=pltpu.VMEM)
    smem = pl.BlockSpec(memory_space=pltpu.SMEM)
    hbm = pl.BlockSpec(memory_space=pltpu.HBM)
    dma = pltpu.SemaphoreType.DMA
    coded = wide + LANES
    r_half, r_cols = n_router // 2, wide // 4
    late = rows * 5 // 11 // 16 * 16
    early = rows - late
    late_a = (late // 16 + 1) // 2 * 16
    clip_limit = 2.0 * math.sqrt(float(GROUPS * units * wide + n_router * wide))
    split = (rows // 16 + 1) // 2 * 16
    state = jax.ShapeDtypeStruct((rows, wide), F32)
    codes = [jax.ShapeDtypeStruct((GROUPS, n, LANES), I16) for n in (rows + 16, rows)]
    weights = jax.ShapeDtypeStruct((units, wide), jnp.bfloat16)
    router_grad, total, weight, new_master, *landed = pl.pallas_call(
        functools.partial(step_kernel, clip_limit),
        out_shape=(
            jax.ShapeDtypeStruct((n_router, wide), F32),
            jax.ShapeDtypeStruct((8, LANES), F32),
            weights,
            state,
            *codes,
        ),
        in_specs=[hbm, hbm, smem, hbm, hbm, hbm, hbm, hbm, smem],
        out_specs=(vmem,) * 6,
        scratch_shapes=[
            dma((3,)),
            pltpu.VMEM((depth, units), jnp.bfloat16),
            pltpu.VMEM((depth, wide), jnp.bfloat16),
            pltpu.VMEM(router_cot.shape, jnp.bfloat16),
            pltpu.VMEM(router_input.shape, jnp.bfloat16),
            pltpu.VMEM((units, depth), jnp.bfloat16),
            pltpu.VMEM((8, rows, wide), F32),
            *[pltpu.VMEM((6, early, coded), I16)] * 2,
            *[pltpu.VMEM((6, late_a, coded), I16)] * 2,
            *[pltpu.VMEM((4, late, coded), I16)] * 2,
            *[pltpu.VMEM((early, coded), I16)] * 2,
            pltpu.VMEM((n_router, wide), F32),
            pltpu.VMEM((r_half, wide), F32),
            pltpu.VMEM((r_half, wide), F32),
            pltpu.VMEM((3, 8, wide), F32),
            pltpu.VMEM((8, wide), F32),
            pltpu.VMEM((3, 8, r_cols), F32),
            pltpu.VMEM((8, r_cols), F32),
            pltpu.VMEM((3, 8, LANES), F32),
            pltpu.VMEM((8, LANES), F32),
            pltpu.VMEM((16, 8, LANES), F32),
            pltpu.VMEM((8, 8, LANES), F32),
            dma((4,)),
            dma((12,)),
            dma((12,)),
            dma((5,)),
            dma((5,)),
            dma((8, 4)),
            dma((8, 4)),
            dma((24,)),
            dma((24,)),
            *[pltpu.VMEM((GROUPS, n, LANES), I16) for n in (split + 16, rows - split)] * 5,
            *[pltpu.VMEM((GROUPS, n, LANES), I16) for n in (rows + 16, rows)] * 3,
            dma((3, 2, GROUPS)),
            dma((3, 2, GROUPS)),
            dma((2, 2, GROUPS)),
            dma((2, 2, GROUPS)),
            dma((8, 2)),
            dma((8, 2)),
        ],
        compiler_params=pltpu.CompilerParams(
            collective_id=0, has_side_effects=True, vmem_limit_bytes=44 * 1024 * 1024
        ),
        name="step",
    )(
        in_hbm(hidden[0]),
        in_hbm(upstream[0]),
        token_counts,
        in_hbm(router_cot),
        in_hbm(router_input),
        in_hbm(master[0]),
        in_hbm(first_moment[0]),
        in_hbm(second_moment[0]),
        partner,
    )

    router = jax.ShapeDtypeStruct(router_master.shape, F32)
    weight, new_master, new_first, new_second, *router_outs = pl.pallas_call(
        functools.partial(close_kernel, clip_limit),
        out_shape=(weights, state, state, state, router, router, router),
        in_specs=[vmem] * 9,
        out_specs=[hbm] * 7,
        scratch_shapes=[
            pltpu.VMEM((2, rows, wide), F32),
            pltpu.VMEM((3, *router_master.shape), F32),
            dma((7,)),
        ],
        compiler_params=pltpu.CompilerParams(vmem_limit_bytes=20 * 1024 * 1024),
        name="close",
    )(weight, new_master, *landed, total, router_grad, router_master, router_first, router_second)
    return (weight[None], new_master[None], new_first[None], new_second[None], *router_outs)


def solution(mesh):
    split = Mesh(mesh.devices.reshape(2, 4, mesh.shape["expert"]), ALL)
    return jax.shard_map(
        on_device,
        mesh=split,
        in_specs=(
            P("e", DP, None),
            P("e", DP, None),
            P("e", DP),
            P("e", DP, None),
            P("e", DP, None),
            P("e", DP, None),
            P(ALL, None),
            P(None, ALL),
            P(),
            P(),
            P(),
            P(),
        ),
        out_specs=(
            P("e", None, None),
            P("e", DP, None),
            P("e", DP, None),
            P("e", DP, None),
            P(),
            P(),
            P(),
        ),
        check_vma=False,
    )
```

```python
import functools
import math

import jax
import jax.numpy as jnp
from jax import lax
from jax.experimental import pallas as pl
from jax.experimental.pallas import tpu as pltpu
from jax.sharding import Mesh
from jax.sharding import PartitionSpec as P

MESH = pl.DeviceIdType.MESH
DP = ("zl", "x")
ALL = ("zl", "x", "e")
F32 = jnp.float32
I16 = jnp.int16

beta_first = 0.9
beta_second = 0.95
learn_rate = 0.001
decay_weight = 0.1
adam_eps = 1e-08
norm_eps = 1e-06
correct_first = 1.0 - 0.9**10
correct_second = 1.0 - 0.95**10

GROUPS = 16
LANES = 128
TOP = 15.0
SMALL = 2.0**-100
MOVE_SCRATCH = 22


def code_of(peak):
    return jnp.ceil(16.0 * jnp.log2(jnp.maximum(peak, SMALL)))


def to_codes(values, code):
    scaled = jnp.round(values * jnp.exp2(TOP - code * (1.0 / 16.0)))
    return jnp.clip(scaled, -32767.0, 32767.0).astype(I16)


def scale_of(code):
    return jnp.exp2(code * (1.0 / 16.0) - TOP)


def encode_rows(values, dst, rows):
    width = values.shape[1]
    code = code_of(jnp.max(jnp.abs(values), axis=1, keepdims=True))
    dst[rows, :width] = to_codes(values, code)
    dst[rows, width:] = jnp.broadcast_to(code, (values.shape[0], LANES)).astype(I16)


def decode_rows(src, rows, width):
    code = src[rows, width : width + LANES].astype(F32)[:, :1]
    return src[rows, :width].astype(F32) * scale_of(code)


def send(src, dst, send_sem, recv_sem, device):
    copy = pltpu.make_async_remote_copy(
        src_ref=src, dst_ref=dst, send_sem=send_sem, recv_sem=recv_sem, device_id=device, device_id_type=MESH
    )
    copy.start()
    return copy


def each(act, start=1):
    def step(j, carry):
        act(j * (GROUPS - 1) % GROUPS)
        return carry

    lax.fori_loop(start, GROUPS, step, 0)


def reduce_kernel(
    states,
    hid_hbm,
    up_hbm,
    counts,
    cot_hbm,
    rin_hbm,
    rgrad,
    total,
    hid,
    up,
    cot,
    rin,
    hid_t,
    terms,
    x_out,
    x_in,
    late_out,
    late_in,
    z_out,
    z_in,
    last_out,
    last_in,
    rp,
    r_in0,
    r1,
    r_in1,
    r2,
    r_in2,
    r3,
    r_in3,
    piece,
    plane_sums,
    side_sums,
    load_sem,
    x_ssem,
    x_rsem,
    z_ssem,
    z_rsem,
    r_ssem,
    r_rsem,
    n_ssem,
    n_rsem,
):
    zl, x, e = (lax.axis_index(a) for a in ALL)
    y, zh, core = e // 4, (e // 2) % 2, e % 2
    z = zh * 2 + zl
    depth, units = hid.shape
    wide = up.shape[1]
    rows = units // 8
    early = x_out.shape[1]
    late = rows - early
    late_a = late_out.shape[1]
    late_b = late - late_a

    def at_x(j):
        return {"x": (x + j) % 4}

    def at_z(j):
        there = (z + j) % 4
        return {"zl": there % 2, "e": y * 4 + (there // 2) * 2 + core}

    def at_y(j):
        return {"e": ((y + j) % 4) * 4 + zh * 2 + core}

    def at_core(j):
        return {"e": e + 1 - 2 * core}

    pair = {"zl": 1 - zl}

    def at_plane(j):
        there = (z + j % 4) % 4
        return {"x": (x + j // 4) % 4, "zl": there % 2, "e": y * 4 + (there // 2) * 2 + core}

    def at_side(j):
        return {"e": ((y + j // 2) % 4) * 4 + zh * 2 + (core + j) % 2}

    loads = [
        pltpu.make_async_copy(src, dst, load_sem.at[n])
        for n, (src, dst) in enumerate(((hid_hbm, hid), (up_hbm, up), (cot_hbm, cot), (rin_hbm, rin)))
    ]
    for copy in loads:
        copy.start()
    barrier = pltpu.get_barrier_semaphore()
    for j in range(1, 16):
        pl.semaphore_signal(barrier, inc=1, device_id=at_plane(j), device_id_type=MESH)

    def greet(device):
        pl.semaphore_signal(barrier, inc=1, device_id=device, device_id_type=MESH)

    each(lambda j: greet({"e": (e + j) % GROUPS}))
    each(lambda j: greet({"e": (e + j) % GROUPS, "zl": 1 - zl}), 0)

    live = counts[0, 0]
    keep = (lax.broadcasted_iota(jnp.int32, (depth, LANES), 0) < live).astype(F32).astype(jnp.bfloat16)
    loads[0].wait()

    @pl.loop(0, units // LANES)
    def _(t):
        cols = pl.ds(pl.multiple_of(t * LANES, LANES), LANES)
        hid_t[cols, :] = (hid[:, cols] * keep).T

    def multiply(block):
        at = pl.multiple_of(block * rows, 16)

        @pl.loop(0, wide // 512)
        def _(n):
            cols = pl.ds(pl.multiple_of(n * 512, 512), 512)
            terms[block, :, cols] = jnp.dot(hid_t[pl.ds(at, rows), :], up[:, cols], preferred_element_type=F32)

    def tiles(start, size, act):
        @pl.loop(0, size // 16, unroll=True)
        def _(i):
            act(
                pl.ds(pl.multiple_of(start + i * 16, 16), 16),
                pl.ds(pl.multiple_of(i * 16, 16), 16),
            )

    def x_made(slot, device):
        return pltpu.make_async_remote_copy(
            src_ref=x_out.at[slot],
            dst_ref=x_in.at[slot],
            send_sem=x_ssem.at[slot],
            recv_sem=x_rsem.at[slot],
            device_id=device,
            device_id_type=MESH,
        )

    def x_copy(slot, device):
        copy = x_made(slot, device)
        copy.start()
        return copy

    def late_copy(slot, size, device):
        r = pl.ds(0, size)
        return send(
            late_out.at[slot, r], late_in.at[slot, r], x_ssem.at[6 + slot], x_rsem.at[6 + slot], device
        )

    def early_part(block, slot, step, incoming=None):
        def act(r, i):
            values = terms[block, r, :]
            if incoming is not None:
                values = values + decode_rows(x_in.at[incoming], i, wide)
            encode_rows(values, x_out.at[slot], i)

        tiles(0, early, act)
        return x_copy(slot, at_x(step))

    def pair_part(n, there):
        def act(r, i):
            encode_rows(terms[(1 - zl) * 4 + there, r, :], z_out.at[n], i)

        tiles(early, late, act)
        return send(z_out.at[n], z_in.at[n], z_ssem.at[n], z_rsem.at[n], pair)

    def pair_sum(n, there):
        block = zl * 4 + there

        def act(r, i):
            terms[block, r, :] += decode_rows(z_in.at[n], i, wide)

        tiles(early, late, act)

    def late_part(there, start, size, slot, step, incoming=None):
        block = zl * 4 + there

        def act(r, i):
            values = terms[block, r, :]
            if incoming is not None:
                values = values + decode_rows(late_in.at[incoming], i, wide)
            encode_rows(values, late_out.at[slot], i)

        tiles(start, size, act)
        return late_copy(slot, size, at_x(step))

    far, right, left = (x + 2) % 4, (x + 1) % 4, (x + 3) % 4
    a_at, b_at = early, early + late_a

    loads[1].wait()
    multiply((1 - zl) * 4 + far)
    pl.semaphore_wait(barrier, 15 + 15 + 16)
    p0 = pair_part(0, far)
    early_part((1 - zl) * 4 + far, 1 - zl, 1 + 2 * zl)
    multiply(zl * 4 + far)
    early_part(zl * 4 + far, zl, 3 - 2 * zl)
    e0, e1 = x_made(0, at_x(3)), x_made(1, at_x(1))
    multiply(right)
    e2 = early_part(right, 2, 1)
    multiply(4 + left)
    e3 = early_part(4 + left, 3, 3)
    multiply(4 + right)
    p1 = pair_part(1, right)

    loads[2].wait()
    loads[3].wait()
    rp[...] = jnp.dot(cot[...], rin[...], preferred_element_type=F32)
    n_router = rp.shape[0]
    r_half, r_cols = n_router // 2, wide // 4
    s0 = send(
        rp.at[pl.ds(pl.multiple_of((1 - core) * r_half, 8), r_half)],
        r_in0,
        r_ssem.at[0, 1],
        r_rsem.at[0, 1],
        at_core(1),
    )
    multiply(left)
    p2 = pair_part(2, left)
    s0.wait_recv()
    r1[...] = rp[pl.ds(pl.multiple_of(core * r_half, 8), r_half), :] + r_in0[...]
    s1 = [
        send(
            r1.at[pl.ds(pl.multiple_of(((y + j) % 4) * 8, 8), 8)],
            r_in1.at[j - 1],
            r_ssem.at[1, j],
            r_rsem.at[1, j],
            at_y(j),
        )
        for j in range(1, 4)
    ]
    multiply(x)
    multiply(4 + x)
    p3 = pair_part(3, x)

    e0.wait_recv()
    e4 = early_part(left, 4, 3, 0)
    e1.wait_recv()
    e5 = early_part(4 + right, 5, 1, 1)
    p0.wait_recv()
    pair_sum(0, far)
    l0 = late_part(far, a_at, late_a, 0, 3)
    l1 = late_part(far, b_at, late_b, 1, 1)

    held = [terms.at[block] for block in (far, 4 + far, (1 - zl) * 4 + right)]
    state_loads = [pltpu.make_async_copy(src, dst, states[3].at[k]) for k, (src, dst) in enumerate(zip(states, held))]
    for copy in state_loads:
        copy.start()

    for copy in s1:
        copy.wait_recv()
    r2[...] = r1[pl.ds(pl.multiple_of(y * 8, 8), 8), :] + r_in1[0] + r_in1[1] + r_in1[2]
    s2 = [
        send(
            r2.at[:, pl.ds(pl.multiple_of(((z + j) % 4) * r_cols, LANES), r_cols)],
            r_in2.at[j - 1],
            r_ssem.at[2, j],
            r_rsem.at[2, j],
            at_z(j),
        )
        for j in range(1, 4)
    ]
    p1.wait_recv()
    pair_sum(1, right)
    l2 = late_part(right, a_at, late_a, 2, 1)
    for copy in s2:
        copy.wait_recv()
    r3[...] = r2[:, pl.ds(pl.multiple_of(z * r_cols, LANES), r_cols)] + r_in2[0] + r_in2[1] + r_in2[2]
    s3 = [
        send(
            r3.at[:, pl.ds(pl.multiple_of(((x + j) % 4) * LANES, LANES), LANES)],
            r_in3.at[j - 1],
            r_ssem.at[3, j],
            r_rsem.at[3, j],
            at_x(j),
        )
        for j in range(1, 4)
    ]
    p2.wait_recv()
    pair_sum(2, left)
    l3 = late_part(left, b_at, late_b, 3, 3)

    for copy in (e2, e3, e4, e5):
        copy.wait_recv()

    def fold(r, i):
        terms[x, r, :] += decode_rows(x_in.at[2], i, wide) + decode_rows(x_in.at[4], i, wide)
        terms[4 + x, r, :] += decode_rows(x_in.at[3], i, wide) + decode_rows(x_in.at[5], i, wide)
        encode_rows(terms[(1 - zl) * 4 + x, r, :], last_out, i)

    tiles(0, early, fold)
    last = send(last_out, last_in, z_ssem.at[4], z_rsem.at[4], pair)
    for copy in s3:
        copy.wait_recv()
    piece[...] = r3[:, pl.ds(pl.multiple_of(x * LANES, LANES), LANES)] + r_in3[0] + r_in3[1] + r_in3[2]
    my_row = core * r_half + y * 8
    z_col = z * r_cols
    x_col = z_col + x * LANES
    rgrad[pl.ds(pl.multiple_of(my_row, 8), 8), pl.ds(pl.multiple_of(x_col, LANES), LANES)] = piece[...]

    def give_back(stage, row, height, col, width, at, size):
        part = rgrad.at[pl.ds(pl.multiple_of(row, 8), height), pl.ds(pl.multiple_of(col, LANES), width)]
        return [
            send(part, part, r_ssem.at[stage, j], r_rsem.at[stage, j], at(j)) for j in range(1, size)
        ]

    b0 = give_back(4, my_row, 8, x_col, LANES, at_x, 4)


    l0.wait_recv()
    l4 = late_part(left, a_at, late_a, 4, 3, 0)
    l1.wait_recv()
    l5 = late_part(right, b_at, late_b, 5, 1, 1)
    p3.wait_recv()
    pair_sum(3, x)
    for copy in b0:
        copy.wait_recv()
    b1 = give_back(5, my_row, 8, z_col, r_cols, at_z, 4)

    own = zl * 4 + x

    def count(values, acc):
        values = values * values
        for a in range(2):
            for b in range(wide // LANES):
                acc = acc + values[a * 8 : a * 8 + 8, b * LANES : (b + 1) * LANES]
        return acc

    def close(start, size, acc, sources):
        def step(n, acc):
            i = pl.ds(pl.multiple_of(n * 16, 16), 16)
            r = pl.ds(pl.multiple_of(start + n * 16, 16), 16)
            values = terms[own, r, :]
            for source in sources:
                values = values + decode_rows(source, i, wide)
            terms[own, r, :] = values
            return count(values, acc)

        return lax.fori_loop(0, size // 16, step, acc, unroll=True)

    squares = jnp.zeros((8, LANES), F32)
    last.wait_recv()
    squares = close(0, early, squares, (last_in,))
    for copy in b1:
        copy.wait_recv()
    b2 = give_back(6, my_row, 8, 0, wide, at_y, 4)
    for copy in (l2, l4):
        copy.wait_recv()
    squares = close(a_at, late_a, squares, (late_in.at[2], late_in.at[4]))
    for copy in (l3, l5):
        copy.wait_recv()
    squares = close(b_at, late_b, squares, (late_in.at[3], late_in.at[5]))

    squares = squares + piece[...] * piece[...]

    def tell(buf, here, at, size, sem):
        buf[here] = squares
        mine = buf.at[here]
        return [send(mine, mine, n_ssem.at[sem + j], n_rsem.at[sem + j], at(j)) for j in range(1, size)]

    def sum_of(buf, size, group):
        for copy in group:
            copy.wait_recv()
        acc = buf[0]
        for k in range(1, size):
            acc = acc + buf[k]
        return acc

    plane_copies = tell(plane_sums, x * 4 + z, at_plane, 16, 0)
    for copy in b2:
        copy.wait_recv()
    b3 = give_back(7, core * r_half, r_half, 0, wide, at_core, 2)
    squares = sum_of(plane_sums, 16, plane_copies)
    side_copies = tell(side_sums, y * 2 + core, at_side, 8, 16)
    squares = sum_of(side_sums, 8, side_copies)
    total[...] = jnp.broadcast_to(jnp.sum(squares), total.shape)
    for copy in b3:
        copy.wait_recv()
    waits = [e0, e1, e2, e3, e4, e5, l0, l1, l2, l3, l4, l5, p0, p1, p2, p3, last, s0, *s1, *s2, *s3]
    for copy in waits + b0 + b1 + b2 + b3 + plane_copies + side_copies:
        copy.wait_send()
    return state_loads, terms.at[own], held


def step_kernel(limit, *refs):
    (hid, up, counts, cot, rin, master_hbm, first_hbm, second_hbm, partner), refs = refs[:9], refs[9:]
    (rgrad, total, weight, new_master, landed0, landed1), refs = refs[:6], refs[6:]
    state_sem, refs = refs[0], refs[1:]
    n = len(refs) - MOVE_SCRATCH
    states = (master_hbm, first_hbm, second_hbm, state_sem)
    loads, grad, held = reduce_kernel(states, hid, up, counts, cot, rin, rgrad, total, *refs[:n])
    for copy in loads:
        copy.wait()
    outs = (weight, new_master, landed0, landed1)
    move_kernel(limit, grad, total, *held, partner, *outs, *refs[n:])


def adam_update(gradient, moment_one, moment_two, weights):
    first_new = beta_first * moment_one + (1.0 - beta_first) * gradient
    second_new = beta_second * moment_two + (1.0 - beta_second) * gradient * gradient
    ratio = first_new / correct_first / (jnp.sqrt(second_new / correct_second) + adam_eps)
    weights_new = weights - learn_rate * (ratio + decay_weight * weights)
    return (weights_new, first_new, second_new)


def in_hbm(array):
    return pltpu.with_memory_space_constraint(array, pltpu.HBM)


def unpack(piece, size, codes):
    return piece[0:size, :].astype(F32) * scale_of(codes.astype(F32))


def close_kernel(
    limit,
    weight,
    new_master,
    landed0,
    landed1,
    total,
    rgrad,
    r_master,
    r_first,
    r_second,
    weight_out,
    master_out,
    first_out,
    second_out,
    r_master_out,
    r_first_out,
    r_second_out,
    values,
    r_values,
    sem,
):
    rows = new_master.shape[0]
    copies = []

    def put(src, dst):
        copy = pltpu.make_async_copy(src, dst, sem.at[len(copies)])
        copy.start()
        copies.append(copy)

    put(weight, weight_out)
    put(new_master, master_out)
    for k, (landed, out) in enumerate(((landed0, first_out), (landed1, second_out))):
        for g in range(GROUPS):
            code = landed0[g, rows + 8 * k : rows + 8 * k + 1, :]
            values[k, :, g * LANES : (g + 1) * LANES] = unpack(landed.at[g], rows, code)
        put(values.at[k], out)
    factor = jnp.minimum(1.0, limit / (jnp.sqrt(total[0:1, 0:1]) + norm_eps))
    new = adam_update(factor * rgrad[...], r_first[...], r_second[...], r_master[...])
    for k, out in enumerate((r_master_out, r_first_out, r_second_out)):
        r_values[k] = new[k]
        put(r_values.at[k], out)
    for copy in copies:
        copy.wait()


def move_kernel(
    limit,
    grad,
    total,
    master,
    first,
    second,
    partner,
    weight,
    new_master,
    landed0,
    landed1,
    lead_out0,
    lead_out1,
    lead_mid0,
    lead_mid1,
    lead_turn0,
    lead_turn1,
    lead_land0,
    lead_land1,
    lead_twin0,
    lead_twin1,
    leaving0,
    leaving1,
    middle0,
    middle1,
    turned0,
    turned1,
    l_ssem,
    l_rsem,
    ssem,
    rsem,
    a_ssem,
    a_rsem,
):
    zl, x, e = (lax.axis_index(a) for a in ALL)
    rows, wide = grad.shape
    half = wide // 2
    lead_out, lead_mid = (lead_out0, lead_out1), (lead_mid0, lead_mid1)
    lead_turn, lead_land, lead_twin = (lead_turn0, lead_turn1), (lead_land0, lead_land1), (lead_twin0, lead_twin1)
    leaving, middle = (leaving0, leaving1), (middle0, middle1)
    turned, landed = (turned0, turned1), (landed0, landed1)
    split = lead_out0.shape[1] - 16
    runs = ((0, split), (split, rows - split))

    def peer(j):
        return {"e": (e + j) % GROUPS}

    def twin_peer(j):
        return {"e": (e + j) % GROUPS, "zl": 1 - zl}

    def at_x(j):
        return {"x": (x + j) % 4}

    factor = jnp.minimum(1.0, limit / (jnp.sqrt(total[0:1, 0:1]) + norm_eps))

    def columns(g):
        return pl.ds(pl.multiple_of(g * LANES, LANES), LANES)

    def update(g):
        c = columns(g)
        return adam_update(factor * grad[:, c], first[:, c], second[:, c], master[:, c])

    def column_code(values):
        return code_of(jnp.max(jnp.abs(values), axis=0, keepdims=True))

    def pack_lead(g):
        values = update(g)[0]
        code = column_code(values)
        for h, (start, size) in enumerate(runs):
            lead_out[h][g, 0:size, :] = to_codes(values[start : start + size], code)
        lead_out[0][g, split:, :] = jnp.broadcast_to(code, (16, LANES)).astype(I16)

    def remote(src, dst, send_sem, recv_sem, device):
        return pltpu.make_async_remote_copy(
            src_ref=src,
            dst_ref=dst,
            send_sem=send_sem,
            recv_sem=recv_sem,
            device_id=device,
            device_id_type=MESH,
        )

    def lead_go(h, j):
        at = (0, h, j)
        return remote(lead_out[h].at[(e + j) % GROUPS], lead_mid[h].at[j], l_ssem.at[at], l_rsem.at[at], peer(j))

    def lead_come(h, j):
        at = (1, h, j)
        src = lead_turn[h].at[(e + j) % GROUPS]
        return remote(src, lead_land[h].at[e], l_ssem.at[at], l_rsem.at[at], peer(j))

    def lead_cross(h, j):
        at = (2, h, j)
        src = lead_turn[h].at[(e + j) % GROUPS]
        return remote(src, lead_twin[h].at[e], l_ssem.at[at], l_rsem.at[at], twin_peer(j))

    def go(k, j):
        at = (0, k, j)
        return remote(leaving[k].at[(e + j) % GROUPS], middle[k].at[j], ssem.at[at], rsem.at[at], peer(j))

    def come(k, j):
        at = (1, k, j)
        return remote(turned[k].at[(e + j) % GROUPS], landed[k].at[e], ssem.at[at], rsem.at[at], peer(j))

    def permute(arrived, to):
        def step(p, carry):
            to[p] = arrived[(e - partner[p] + GROUPS) % GROUPS]
            return carry

        lax.fori_loop(0, GROUPS, step, 0)

    pack_lead(e)

    def first_leg(j):
        pack_lead((e + j) % GROUPS)
        lead_go(0, j).start()

    each(first_leg)
    each(lambda j: lead_go(1, j).start())
    for h in range(2):
        lead_mid[h][0] = lead_out[h][e]

    for h in range(2):
        each(lambda j, h=h: lead_go(h, j).wait_recv())
        permute(lead_mid[h], lead_turn[h])
        each(lambda j, h=h: lead_come(h, j).start())
        lead_land[h][e] = lead_turn[h][e]
    for h in range(2):
        each(lambda j, h=h: lead_cross(h, j).start(), 0)

    def moments(g):
        _, first_new, second_new = update(g)
        code = column_code(first_new), column_code(second_new)
        leaving0[g, 0:rows, :] = to_codes(first_new, code[0])
        leaving1[g] = to_codes(second_new, code[1])
        both = [jnp.broadcast_to(c, (8, LANES)) for c in code]
        leaving0[g, rows:, :] = jnp.concatenate(both, axis=0).astype(I16)

    each(moments, 0)

    own, twin = zl * 4 + x, (1 - zl) * 4 + x
    left, right = (x + 3) % 4, (x + 1) % 4

    def weight_rows(block, h):
        return pl.ds(pl.multiple_of(block * rows + runs[h][0], 16), runs[h][1])

    def gather(n, h, block, col, width, device):
        part = weight.at[weight_rows(block, h), pl.ds(col, width)]
        return send(part, part, a_ssem.at[n, h], a_rsem.at[n, h], device)

    def settle(h, g):
        values = unpack(lead_land[h].at[g], runs[h][1], lead_land0[g, split : split + 1, :])
        new_master[pl.ds(*runs[h]), columns(g)] = values
        weight[weight_rows(own, h), columns(g)] = values.astype(jnp.bfloat16)

    def settle_twin(h, g):
        values = unpack(lead_twin[h].at[g], runs[h][1], lead_twin0[g, split : split + 1, :])
        weight[weight_rows(twin, h), columns(g)] = values.astype(jnp.bfloat16)

    to_right, to_left = [], []
    for h in range(2):
        settle(h, e)

        def settle_next(j, h=h):
            lead_come(h, j).wait_recv()
            settle(h, (e - j + GROUPS) % GROUPS)

        each(settle_next)
        to_right.append(gather(0, h, own, 0, wide, at_x(1)))
        to_left.append(gather(1, h, own, 0, wide, at_x(3)))

    each(lambda j: go(0, j).start())
    each(lambda j: go(1, j).start())

    twin_right, twin_left = [], []
    for h in range(2):

        def settle_cross(j, h=h):
            lead_cross(h, j).wait_recv()
            settle_twin(h, (e - j + GROUPS) % GROUPS)

        each(settle_cross, 0)
        twin_right.append(gather(2, h, twin, 0, wide, at_x(1)))
        twin_left.append(gather(3, h, twin, 0, wide, at_x(3)))

    onward = []

    def pass_on(n, h, z_at, from_left, from_right):
        from_left.wait_recv()
        onward.append(gather(n, h, z_at * 4 + left, 0, half, at_x(1)))
        from_right.wait_recv()
        onward.append(gather(n + 1, h, z_at * 4 + right, half, half, at_x(3)))

    def turn(k):
        each(lambda j: go(k, j).wait_recv())
        middle[k][0] = leaving[k][e]
        permute(middle[k], turned[k])
        each(lambda j: come(k, j).start())
        landed[k][e] = turned[k][e]

    pass_on(4, 0, zl, to_right[0], to_left[0])
    pass_on(4, 1, zl, to_right[1], to_left[1])
    turn(0)
    pass_on(6, 0, 1 - zl, twin_right[0], twin_left[0])
    turn(1)
    pass_on(6, 1, 1 - zl, twin_right[1], twin_left[1])

    for k in range(2):
        each(lambda j, k=k: come(k, j).wait_recv())
    for copy in onward:
        copy.wait_recv()
    for k in range(2):
        each(lambda j, k=k: lead_go(k, j).wait_send())
        each(lambda j, k=k: lead_come(k, j).wait_send())
        each(lambda j, k=k: lead_cross(k, j).wait_send(), 0)
        each(lambda j, k=k: go(k, j).wait_send())
        each(lambda j, k=k: come(k, j).wait_send())
    for copy in to_right + to_left + twin_right + twin_left + onward:
        copy.wait_send()


def on_device(
    hidden,
    upstream,
    token_counts,
    master,
    first_moment,
    second_moment,
    router_input,
    router_cot,
    router_master,
    router_first,
    router_second,
    partner,
):
    depth, units = hidden.shape[1:]
    wide = upstream.shape[2]
    rows = units // 8
    n_router = router_cot.shape[0]
    vmem = pl.BlockSpec(memory_space=pltpu.VMEM)
    smem = pl.BlockSpec(memory_space=pltpu.SMEM)
    hbm = pl.BlockSpec(memory_space=pltpu.HBM)
    dma = pltpu.SemaphoreType.DMA
    coded = wide + LANES
    r_half, r_cols = n_router // 2, wide // 4
    late = rows * 5 // 11 // 16 * 16
    early = rows - late
    late_a = (late // 16 + 1) // 2 * 16
    clip_limit = 2.0 * math.sqrt(float(GROUPS * units * wide + n_router * wide))
    split = (rows // 16 + 1) // 2 * 16
    state = jax.ShapeDtypeStruct((rows, wide), F32)
    codes = [jax.ShapeDtypeStruct((GROUPS, n, LANES), I16) for n in (rows + 16, rows)]
    weights = jax.ShapeDtypeStruct((units, wide), jnp.bfloat16)
    router_grad, total, weight, new_master, *landed = pl.pallas_call(
        functools.partial(step_kernel, clip_limit),
        out_shape=(
            jax.ShapeDtypeStruct((n_router, wide), F32),
            jax.ShapeDtypeStruct((8, LANES), F32),
            weights,
            state,
            *codes,
        ),
        in_specs=[hbm, hbm, smem, hbm, hbm, hbm, hbm, hbm, smem],
        out_specs=(vmem,) * 6,
        scratch_shapes=[
            dma((3,)),
            pltpu.VMEM((depth, units), jnp.bfloat16),
            pltpu.VMEM((depth, wide), jnp.bfloat16),
            pltpu.VMEM(router_cot.shape, jnp.bfloat16),
            pltpu.VMEM(router_input.shape, jnp.bfloat16),
            pltpu.VMEM((units, depth), jnp.bfloat16),
            pltpu.VMEM((8, rows, wide), F32),
            *[pltpu.VMEM((6, early, coded), I16)] * 2,
            *[pltpu.VMEM((6, late_a, coded), I16)] * 2,
            *[pltpu.VMEM((4, late, coded), I16)] * 2,
            *[pltpu.VMEM((early, coded), I16)] * 2,
            pltpu.VMEM((n_router, wide), F32),
            pltpu.VMEM((r_half, wide), F32),
            pltpu.VMEM((r_half, wide), F32),
            pltpu.VMEM((3, 8, wide), F32),
            pltpu.VMEM((8, wide), F32),
            pltpu.VMEM((3, 8, r_cols), F32),
            pltpu.VMEM((8, r_cols), F32),
            pltpu.VMEM((3, 8, LANES), F32),
            pltpu.VMEM((8, LANES), F32),
            pltpu.VMEM((16, 8, LANES), F32),
            pltpu.VMEM((8, 8, LANES), F32),
            dma((4,)),
            dma((12,)),
            dma((12,)),
            dma((5,)),
            dma((5,)),
            dma((8, 4)),
            dma((8, 4)),
            dma((24,)),
            dma((24,)),
            *[pltpu.VMEM((GROUPS, n, LANES), I16) for n in (split + 16, rows - split)] * 5,
            *[pltpu.VMEM((GROUPS, n, LANES), I16) for n in (rows + 16, rows)] * 3,
            dma((3, 2, GROUPS)),
            dma((3, 2, GROUPS)),
            dma((2, 2, GROUPS)),
            dma((2, 2, GROUPS)),
            dma((8, 2)),
            dma((8, 2)),
        ],
        compiler_params=pltpu.CompilerParams(
            collective_id=0, has_side_effects=True, vmem_limit_bytes=44 * 1024 * 1024
        ),
        name="step",
    )(
        in_hbm(hidden[0]),
        in_hbm(upstream[0]),
        token_counts,
        in_hbm(router_cot),
        in_hbm(router_input),
        in_hbm(master[0]),
        in_hbm(first_moment[0]),
        in_hbm(second_moment[0]),
        partner,
    )

    router = jax.ShapeDtypeStruct(router_master.shape, F32)
    weight, new_master, new_first, new_second, *router_outs = pl.pallas_call(
        functools.partial(close_kernel, clip_limit),
        out_shape=(weights, state, state, state, router, router, router),
        in_specs=[vmem] * 9,
        out_specs=[hbm] * 7,
        scratch_shapes=[
            pltpu.VMEM((2, rows, wide), F32),
            pltpu.VMEM((3, *router_master.shape), F32),
            dma((7,)),
        ],
        compiler_params=pltpu.CompilerParams(vmem_limit_bytes=20 * 1024 * 1024),
        name="close",
    )(weight, new_master, *landed, total, router_grad, router_master, router_first, router_second)
    return (weight[None], new_master[None], new_first[None], new_second[None], *router_outs)


def solution(mesh):
    split = Mesh(mesh.devices.reshape(2, 4, mesh.shape["expert"]), ALL)
    return jax.shard_map(
        on_device,
        mesh=split,
        in_specs=(
            P("e", DP, None),
            P("e", DP, None),
            P("e", DP),
            P("e", DP, None),
            P("e", DP, None),
            P("e", DP, None),
            P(ALL, None),
            P(None, ALL),
            P(),
            P(),
            P(),
            P(),
        ),
        out_specs=(
            P("e", None, None),
            P("e", DP, None),
            P("e", DP, None),
            P("e", DP, None),
            P(),
            P(),
            P(),
        ),
        check_vma=False,
    )
```
